32 devices in a mesh: rep: 2 (over y), seq: 4 (over z), section: 2 (over core), head: 2 (over x).
Axes of the slice: x: 2, y: 2, z: 4, core: 2. Of those that a mesh axis runs over, the one named last changes fastest.
Arguments:
- hidden: bfloat16 [6, 256, 2048], P('rep', 'seq'), parts along dimension 0, may hold values from -6 to 6
- lengths: int32 [6], P('rep'), parts along dimension 0, may hold values from 1 to 256, 576 in all
- attn_gain: float32 [2, 2048], P('section'), may hold values from 0.1 to 1.9
- w_query: bfloat16 [2, 2048, 2048], P('section', None, 'head'), may hold values from -2 to 2
- w_latent: bfloat16 [2, 2048, 512], P('section'), may hold values from -0.125 to 0.125
- latent_gain: float32 [2, 512], P('section'), may hold values from 0.1 to 1.9
- w_key: bfloat16 [2, 512, 2048], P('section', None, 'head'), may hold values from -0.25 to 0.25
- w_value: bfloat16 [2, 512, 2048], P('section', None, 'head'), may hold values from -0.25 to 0.25
- w_out: bfloat16 [2, 2048, 2048], P('section', 'head'), may hold values from -0.125 to 0.125
Outputs:
- final: float32 [6, 256, 2048], P('rep', ('seq', 'head'), 'section'), parts along dimension 0
- latents: float32 [2, 6, 256, 512], P('section', 'rep', 'seq'), parts along dimension 1
The draws below stay inside these ranges and needn't reach their ends.
There are 2 independent parts, one for each index of `rep`. The reference program is written for one: setup_inputs(seed, part) draws one part's arguments, and reference() takes and returns one part's arrays. A program takes and returns all parts, laid end to end along the dimension named above; an argument that names none is the same for every part. Nothing has to cross between parts.
Inputs may be any that keep to these rules, and one draw needn't show every extreme that they name: lengths sum to 576 and one block holds exactly 256; the live tokens of a block are its first slots.
All inputs are finite; a program needn't handle non-finite values.
Results may differ from the reference program's by a relative error of at most 0.015.
The reference program's roundings to bfloat16 on the way (of `normed`, `query`, `latent`, `absorbed`, `rounded`, `context` and `attn`) count: a program that leaves them out, or rounds other values in their place, can miss the bound.
Values may be sent and summed in bfloat16 or wider, within the bound.
A program may use at most 128 MiB of HBM per device.

```python
import math
import jax
import jax.numpy as jnp
import numpy as np
from jax import lax

D = 2048
HEADS = 16
HD = 128
R = 512
GROUPS = 3
TOKC = 256
LAYERS = 2


def draw_w_query(key, part):
    full_shape = (LAYERS, D, HEADS * HD)
    entries = jax.random.truncated_normal(key, -6.0, 6.0, full_shape, jnp.float32) * D ** (-0.5)
    return entries.astype(jnp.bfloat16)


def block_levels(stream_key, dims, cuts, smallest, top_value):
    factor_of = 1.0
    for axis_at, parts in cuts:
        draws = jax.random.uniform(jax.random.fold_in(jax.random.fold_in(stream_key, 6), axis_at), (parts,), jnp.float32, smallest / len(cuts), top_value / len(cuts))
        factor_of = factor_of * jnp.repeat(jnp.exp(draws), dims[axis_at] // parts).reshape((-1,) + (1,) * (len(dims) - 1 - axis_at))
    return factor_of


def length_profile(count, total, most, lean):
    loads = [(1 << 20) // math.isqrt(rank ** lean) + 1 for rank in range(2, count + 1)]
    spare, counts = total - most - (count - 1), [1] * (count - 1)
    while spare > 0:
        candidates = [i for i in range(count - 1) if counts[i] < most]
        pool, left = sum([loads[i] for i in candidates]), spare
        for i in candidates:
            more = min(most - counts[i], max(1, left * loads[i] // pool), spare)
            counts[i] = counts[i] + more
            spare = spare - more
    return np.array([most] + counts)


def uneven_parts(stream_key, number_of, total, bound, slope):
    if number_of == 2:
        one = jax.random.randint(stream_key, (), max(1, total - bound), min(bound, total - 1) + 1)
        return jnp.stack([one, total - one])
    tallies = jnp.asarray(length_profile(number_of, total, bound, slope), jnp.int32)
    twos = (number_of - 1) // 2
    source_of, receiver = tallies[1:1 + 2 * twos:2], tallies[2:2 + 2 * twos:2]
    slack = jnp.minimum(source_of - 1, bound - receiver)
    shifted = jax.random.randint(jax.random.fold_in(stream_key, 1), (twos,), 0, 1 << 20) % (slack + 1)
    tallies = tallies.at[1:1 + 2 * twos:2].set(source_of - shifted).at[2:2 + 2 * twos:2].set(receiver + shifted)
    return tallies[jax.random.permutation(jax.random.fold_in(stream_key, 2), number_of)]


def bell_draw(rng, extent, scale, bound, cuts=(), kind=jnp.bfloat16):
    values = scale * jax.random.normal(rng, extent, jnp.float32)
    if cuts:
        values = values * block_levels(rng, extent, cuts, -0.22, 0.18)
    return jnp.clip(values, -bound, bound).astype(kind)


def setup_inputs(seed: int = 0, part: int = 0) -> dict:
    streams_of = jax.random.split(jax.random.key(seed), 10)
    part_splits = jax.random.split(jax.random.fold_in(streams_of[9], part), 10)
    return {
        "hidden": bell_draw(part_splits[0], (GROUPS, TOKC, D), 1.0, 6.0, ((1, 4),)),
        "lengths": uneven_parts(part_splits[1], GROUPS, 3 * GROUPS * TOKC // 4, TOKC, 2).astype(jnp.int32),
        "attn_gain": jnp.clip(1.0 + 0.18 * jax.random.normal(streams_of[2], (LAYERS, D), jnp.float32), 0.1, 1.9),
        "w_query": draw_w_query(jax.random.fold_in(streams_of[9], 71), part),
        "w_latent": bell_draw(streams_of[4], (LAYERS, D, R), D ** -0.5, 0.125, ((0, 2),)),
        "latent_gain": jnp.clip(1.0 + 0.18 * jax.random.normal(streams_of[5], (LAYERS, R), jnp.float32), 0.1, 1.9),
        "w_key": bell_draw(streams_of[6], (LAYERS, R, HEADS * HD), R ** -0.5, 0.25, ((0, 2), (2, 2))),
        "w_value": bell_draw(streams_of[7], (LAYERS, R, HEADS * HD), R ** -0.5, 0.25, ((0, 2), (2, 2))),
        "w_out": bell_draw(streams_of[8], (LAYERS, HEADS * HD, D), (HEADS * HD) ** -0.5, 0.125, ((0, 2), (1, 2))),
    }


def rms_scale(values, gain):
    values = values.astype(jnp.float32)
    mean_sq = lax.optimization_barrier(jnp.mean(values * values, axis=-1, keepdims=True))
    return values * lax.rsqrt(mean_sq + 1e-06) * gain

def reference(hidden, lengths, attn_gain, w_query, w_latent, latent_gain, w_key, w_value, w_out):
    groups, group_rows, width = hidden.shape
    heads = w_key.shape[2] // HD
    rank = w_latent.shape[2]
    position = jnp.arange(group_rows, dtype=jnp.int32)
    block_ids = jnp.arange(groups, dtype=jnp.int32)
    live = position[None, :] < lengths[:, None]
    scale = 1.0 / HD ** 0.5
    state = hidden.astype(jnp.float32)
    stored = []
    for layer in range(LAYERS):
        normed = rms_scale(state, attn_gain[layer]).astype(jnp.bfloat16)
        flat = normed.reshape(groups * group_rows, width)
        query = jnp.dot(flat, w_query[layer], preferred_element_type=jnp.float32).astype(jnp.bfloat16)
        query = query.reshape(groups, group_rows, heads, HD)
        raw = jnp.dot(flat, w_latent[layer], preferred_element_type=jnp.float32)
        latent_full = rms_scale(raw, latent_gain[layer]).reshape(groups, group_rows, rank)
        latent = latent_full.astype(jnp.bfloat16)
        key_map = w_key[layer].astype(jnp.float32).reshape(rank, heads, HD)
        value_map = w_value[layer].astype(jnp.float32).reshape(rank, heads, HD)
        latent_wide = lax.optimization_barrier(latent).astype(jnp.float32)
        pieces = []
        for group in range(groups):
            seen = group + 1
            absorbed = (jnp.einsum('qhd,rhd->hqr', query[group].astype(jnp.float32), key_map) * scale).astype(jnp.bfloat16)
            absorbed_wide = lax.optimization_barrier(absorbed).astype(jnp.float32)
            keys_seen = latent_wide[:seen]
            scores = jnp.einsum('hqr,ckr->hqck', absorbed_wide, keys_seen)
            ids = block_ids[:seen]
            past = (ids < group)[:, None] & live[:seen]
            same = (ids == group)[None, :, None] & (position[None, None, :] <= position[:, None, None])
            mask = past[None] | same
            scores = jnp.where(mask[None], scores, -1e+30)
            top = lax.optimization_barrier(jnp.max(scores, axis=(2, 3), keepdims=True))
            weights = jnp.where(mask[None], jnp.exp(scores - top), 0.0)
            total = lax.optimization_barrier(jnp.sum(weights, axis=(2, 3)))
            rounded = lax.optimization_barrier(weights.astype(jnp.bfloat16)).astype(jnp.float32)
            context = jnp.einsum('hqck,ckr->hqr', rounded, keys_seen) / total[:, :, None]
            context = lax.optimization_barrier(context.astype(jnp.bfloat16)).astype(jnp.float32)
            attn = jnp.einsum('hqr,rhd->qhd', context, value_map)
            pieces.append(attn.reshape(group_rows, heads * HD).astype(jnp.bfloat16))
        attn_all = jnp.concatenate(pieces, axis=0)
        update = jnp.dot(attn_all, w_out[layer], preferred_element_type=jnp.float32)
        state = state + update.reshape(groups, group_rows, width)
        stored.append(jnp.where(live[:, :, None], latent_full, jnp.zeros_like(latent_full)))
    final = jnp.where(live[:, :, None], state, jnp.zeros_like(state))
    return (final, jnp.stack(stored, axis=0))
```

```python
import functools

import jax
import jax.numpy as jnp
from jax import lax
from jax.experimental import pallas as pl
from jax.experimental.pallas import tpu as pltpu
from jax.sharding import PartitionSpec as P

HD = 128
MESH = pl.DeviceIdType.MESH
F32 = jnp.float32
BF16 = jnp.bfloat16


def rms_scale(values, gain):
    mean_sq = jnp.mean(values * values, axis=-1, keepdims=True)
    return values * lax.rsqrt(mean_sq + 1e-06) * gain


def dot_nt(a, b):
    return lax.dot_general(a, b, (((1,), (1,)), ((), ())), preferred_element_type=F32)


def kernel(
    dims,
    lengths_h,
    hidden,
    gain_h,
    lgain_h,
    wq,
    wl,
    wk,
    wv,
    wo,
    fin_v,
    lat_f,
    lengths,
    gain,
    lgain,
    hid_v,
    wq_v,
    wl_v,
    wk_v,
    wv_v,
    wo_v,
    x_s,
    normed_s,
    lat_b,
    cache,
    absorbed_s,
    attn_s,
    out_s,
    part_in,
    fin_in,
    load_sem,
    z_send,
    z_recv,
    h_send,
    h_recv,
    f_send,
    f_recv,
):
    seqs, sections, heads = dims
    seq = lax.axis_index("seq")
    sec = lax.axis_index("section")
    head = lax.axis_index("head")
    groups, rows, width = hid_v.shape
    rank = wl_v.shape[1]
    cols = wq_v.shape[1]
    heads_here = cols // HD
    share = rows // heads
    pw = width // sections
    tok = rows * seqs
    scale = 1.0 / HD**0.5
    first_sec = sec == 0
    last_sec = sec == sections - 1

    loads = [
        pltpu.make_async_copy(src, dst, load_sem.at[i])
        for i, (src, dst) in enumerate(
            [
                (hidden, hid_v),
                (wl.at[0], wl_v),
                (wq.at[0], wq_v),
                (wk.at[0], wk_v),
                (wv.at[0], wv_v),
                (wo.at[0], wo_v),
            ]
        )
    ]
    small = [
        pltpu.make_async_copy(src, dst, load_sem.at[6 + i])
        for i, (src, dst) in enumerate([(gain_h, gain), (lgain_h, lgain), (lengths_h, lengths)])
    ]
    loads[0].start()
    for c in small:
        c.start()
    for c in loads[1:]:
        c.start()

    barrier = pltpu.get_barrier_semaphore()
    peers = [{"seq": lax.rem(seq + d, seqs)} for d in range(1, seqs)]
    for ds in range(sections):
        for dh in range(heads):
            if ds or dh:
                peers.append(
                    {
                        "section": lax.rem(sec + ds, sections),
                        "head": lax.rem(head + dh, heads),
                    }
                )
    for peer in peers:
        pl.semaphore_signal(barrier, inc=1, device_id=peer, device_id_type=MESH)

    own = pl.ds(pl.multiple_of(seq * rows, rows), rows)
    pos = seq * rows + lax.broadcasted_iota(jnp.int32, (rows, 1), 0)

    def z_copy(g, d):
        return pltpu.make_async_remote_copy(
            src_ref=lat_b.at[g],
            dst_ref=cache.at[g, own],
            send_sem=z_send.at[g, d - 1],
            recv_sem=z_recv.at[g, d - 1],
            device_id={"seq": lax.rem(seq + d, seqs)},
            device_id_type=MESH,
        )

    def h_copy(g, p, dh):
        return pltpu.make_async_remote_copy(
            src_ref=out_s.at[g, :, pl.ds(p * pw, pw)],
            dst_ref=part_in.at[head, g, :, pl.ds(p * pw, pw)],
            send_sem=h_send.at[g, p, dh],
            recv_sem=h_recv.at[g, p, head],
            device_id={"section": lax.rem(sec + 1, sections), "head": lax.rem(head + dh, heads)},
            device_id_type=MESH,
        )

    def h_arrival(g, p, source):
        return pltpu.make_async_remote_copy(
            src_ref=out_s.at[g, :, pl.ds(p * pw, pw)],
            dst_ref=part_in.at[source, g, :, pl.ds(p * pw, pw)],
            send_sem=h_send.at[g, p, 0],
            recv_sem=h_recv.at[g, p, source],
            device_id={"section": lax.rem(sec + 1, sections)},
            device_id_type=MESH,
        )

    def f_copy(g, ds, dh):
        to_sec = lax.rem(sec + ds, sections)
        to_head = lax.rem(head + dh, heads)
        return pltpu.make_async_remote_copy(
            src_ref=out_s.at[
                g,
                pl.ds(pl.multiple_of(to_head * share, share), share),
                pl.ds(pl.multiple_of(to_sec * pw, pw), pw),
            ],
            dst_ref=fin_in.at[dh, g],
            send_sem=f_send.at[g, ds * heads + dh],
            recv_sem=f_recv.at[g, dh],
            device_id={"section": to_sec, "head": to_head},
            device_id_type=MESH,
        )

    def latent_part(g0, ng):
        span = slice(g0 * rows, (g0 + ng) * rows)
        raw = jnp.dot(normed_s[span], wl_v[...], preferred_element_type=F32)
        full = rms_scale(raw, lgain[...])
        for i in range(ng):
            g = g0 + i
            piece = full[i * rows : (i + 1) * rows]
            narrow = piece.astype(BF16)
            lat_b[g] = narrow
            cache[g, own] = narrow
            lat_f[0, g] = jnp.where(pos < lengths[g], piece, 0.0)

    def latent_send(g):
        for d in range(1, seqs):
            z_copy(g, d).start()

    def query_part(g0, ng):
        span = slice(g0 * rows, (g0 + ng) * rows)
        query = jnp.dot(normed_s[span], wq_v[...], preferred_element_type=F32).astype(BF16)
        for h in range(heads_here):
            at = slice(h * HD, (h + 1) * HD)
            absorbed = (dot_nt(query[:, at], wk_v[:, at]) * scale).astype(BF16)
            for i in range(ng):
                absorbed_s[g0 + i, h * rows : (h + 1) * rows] = absorbed[i * rows : (i + 1) * rows]

    def take_input(g):
        for p in range(sections):
            for source in range(heads):
                h_arrival(g, p, source).wait_recv()
        half = rows // 2
        for r0 in range(0, rows, half):
            r = slice(r0, r0 + half)
            added = part_in[0, g, r].astype(F32)
            for source in range(1, heads):
                added = added + part_in[source, g, r].astype(F32)
            x = hid_v[g, r].astype(F32) + added
            x_s[g, r] = x
            normed_s[g * rows + r0 : g * rows + r0 + half] = rms_scale(x, gain[...]).astype(BF16)

    def project_later(g):
        take_input(g)
        latent_part(g, 1)
        latent_send(g)
        query_part(g, 1)

    loads[0].wait()
    for c in small:
        c.wait()

    @pl.when(first_sec)
    def _():
        half = rows // 2
        for g in range(groups):
            for r0 in range(0, rows, half):
                x = hid_v[g, r0 : r0 + half].astype(F32)
                if sections == 1:
                    x_s[g, r0 : r0 + half] = x
                normed_s[g * rows + r0 : g * rows + r0 + half] = rms_scale(x, gain[...]).astype(
                    BF16
                )
        loads[1].wait()
        latent_part(0, groups)

    pl.semaphore_wait(barrier, len(peers))

    @pl.when(first_sec)
    def _():
        for g in range(groups):
            latent_send(g)
        loads[2].wait()
        loads[3].wait()
        query_part(0, groups)

    @pl.when(jnp.logical_not(first_sec))
    def _():
        for i in range(1, 4):
            loads[i].wait()
        for g in range(min(2, groups)):
            project_later(g)

    loads[4].wait()
    loads[5].wait()

    key_pos = lax.broadcasted_iota(jnp.int32, (1, tok), 1)
    row_in = lax.broadcasted_iota(jnp.int32, (rows, 1), 0)
    mine = (row_in >= head * share) & (row_in < (head + 1) * share)

    def attend(g):
        keys = (g + 1) * tok
        per = heads_here
        while per > 2 and per * rows * keys > 512 * 768:
            per //= 2
        same = jnp.where(key_pos <= pos, 0.0, -1e30)
        same = jnp.concatenate([same] * per, axis=0)
        past = [jnp.where(key_pos < lengths[b], 0.0, -1e30) for b in range(g)]
        for d in range(1, seqs):
            z_copy(g, d).wait_recv()
        for h0 in range(0, heads_here, per):
            span = slice(h0 * rows, (h0 + per) * rows)
            scores = [dot_nt(absorbed_s[g, span], cache[b]) + past[b] for b in range(g)]
            scores.append(dot_nt(absorbed_s[g, span], cache[g]) + same)
            top = jnp.max(scores[0], axis=1, keepdims=True)
            for piece in scores[1:]:
                top = jnp.maximum(top, jnp.max(piece, axis=1, keepdims=True))
            total = None
            accum = None
            for b in range(g + 1):
                weights = jnp.exp(scores[b] - top)
                part = jnp.sum(weights, axis=1, keepdims=True)
                gained = jnp.dot(weights.astype(BF16), cache[b], preferred_element_type=F32)
                total = part if total is None else total + part
                accum = gained if accum is None else accum + gained
            context = (accum / total).astype(BF16)
            for i in range(0, per, 2):
                n = min(2, per - i)
                both = jnp.dot(
                    context[i * rows : (i + n) * rows],
                    wv_v[:, (h0 + i) * HD : (h0 + i + n) * HD],
                    preferred_element_type=F32,
                )
                for j in range(n):
                    at = slice((h0 + i + j) * HD, (h0 + i + j + 1) * HD)
                    attn_s[g, :, at] = both[
                        j * rows : (j + 1) * rows, j * HD : (j + 1) * HD
                    ].astype(BF16)

        step = min(pw, 512)

        @pl.when(jnp.logical_not(last_sec))
        def _():
            for p in range(sections):
                for c0 in range(p * pw, (p + 1) * pw, step):
                    out_s[g, :, c0 : c0 + step] = jnp.dot(
                        attn_s[g], wo_v[:, c0 : c0 + step], preferred_element_type=F32
                    ).astype(BF16)
                for dh in range(heads - 1, -1, -1):
                    h_copy(g, p, dh).start()

        @pl.when(last_sec)
        def _():
            for p in range(sections):
                for c0 in range(p * pw, (p + 1) * pw, step):
                    added = jnp.dot(attn_s[g], wo_v[:, c0 : c0 + step], preferred_element_type=F32)
                    state = x_s[g, :, c0 : c0 + step] + added
                    x_s[g, :, c0 : c0 + step] = state
                    out_s[g, :, c0 : c0 + step] = jnp.where(mine, state, added).astype(BF16)
                ds = (p + 1) % sections
                for dh in range(heads - 1, -1, -1):
                    if ds or dh:
                        f_copy(g, ds, dh).start()

    for g in range(groups):
        attend(g)
        if g + 2 < groups:

            @pl.when(jnp.logical_not(first_sec))
            def _():
                project_later(g + 2)

    out_pos = seq * rows + head * share + lax.broadcasted_iota(jnp.int32, (share, 1), 0)
    my_rows = pl.ds(pl.multiple_of(head * share, share), share)
    my_cols = pl.ds(pl.multiple_of(sec * pw, pw), pw)
    for g in range(groups):
        for dh in range(1, heads):
            f_copy(g, 0, dh).wait_recv()

        @pl.when(last_sec)
        def _():
            fin_v[g] = x_s[g, my_rows, my_cols]

        @pl.when(jnp.logical_not(last_sec))
        def _():
            f_copy(g, 1, 0).wait_recv()
            fin_v[g] = fin_in[0, g].astype(F32)

        value = fin_v[g]
        for dh in range(1, heads):
            value = value + fin_in[dh, g].astype(F32)
        fin_v[g] = jnp.where(out_pos < lengths[g], value, 0.0)

    for g in range(groups):
        for d in range(1, seqs):
            z_copy(g, d).wait_send()

    @pl.when(jnp.logical_not(last_sec))
    def _():
        for g in range(groups):
            for p in range(sections):
                for dh in range(heads):
                    h_copy(g, p, dh).wait_send()

    @pl.when(last_sec)
    def _():
        for g in range(groups):
            for ds in range(sections):
                for dh in range(heads):
                    if ds or dh:
                        f_copy(g, ds, dh).wait_send()


def solution(mesh):
    seqs, sections, heads = mesh.shape["seq"], mesh.shape["section"], mesh.shape["head"]

    def shards(hidden, lengths, attn_gain, w_query, w_latent, latent_gain, w_key, w_value, w_out):
        groups, rows, width = hidden.shape
        rank = w_latent.shape[2]
        cols = w_query.shape[2]
        share, pw = rows // heads, width // sections
        hbm = pl.BlockSpec(memory_space=pltpu.HBM)
        vmem = pl.BlockSpec(memory_space=pltpu.VMEM)
        dma = pltpu.SemaphoreType.DMA
        return pl.pallas_call(
            functools.partial(kernel, (seqs, sections, heads)),
            out_shape=(
                pltpu.VMEM((groups, share, pw), F32),
                pltpu.VMEM((1, groups, rows, rank), F32),
            ),
            in_specs=[hbm] * 9,
            out_specs=(vmem, vmem),
            scratch_shapes=[
                pltpu.SMEM((groups,), jnp.int32),
                pltpu.VMEM((1, width), F32),
                pltpu.VMEM((1, rank), F32),
                pltpu.VMEM((groups, rows, width), BF16),
                pltpu.VMEM((width, cols), BF16),
                pltpu.VMEM((width, rank), BF16),
                pltpu.VMEM((rank, cols), BF16),
                pltpu.VMEM((rank, cols), BF16),
                pltpu.VMEM((cols, width), BF16),
                pltpu.VMEM((groups, rows, width), F32),
                pltpu.VMEM((groups * rows, width), BF16),
                pltpu.VMEM((groups, rows, rank), BF16),
                pltpu.VMEM((groups, rows * seqs, rank), BF16),
                pltpu.VMEM((groups, cols // HD * rows, rank), BF16),
                pltpu.VMEM((groups, rows, cols), BF16),
                pltpu.VMEM((groups, rows, width), BF16),
                pltpu.VMEM((heads, groups, rows, width), BF16),
                pltpu.VMEM((heads, groups, share, pw), BF16),
                dma((9,)),
                dma((groups, max(1, seqs - 1))),
                dma((groups, max(1, seqs - 1))),
                dma((groups, sections, heads)),
                dma((groups, sections, heads)),
                dma((groups, sections * heads)),
                dma((groups, heads)),
            ],
            compiler_params=pltpu.CompilerParams(
                collective_id=0, has_side_effects=True, vmem_limit_bytes=60 * 1024 * 1024
            ),
        )(lengths, hidden, attn_gain, latent_gain, w_query, w_latent, w_key, w_value, w_out)

    return jax.shard_map(
        shards,
        mesh=mesh,
        in_specs=(
            P("rep", "seq", None),
            P("rep"),
            P("section", None),
            P("section", None, "head"),
            P("section", None, None),
            P("section", None),
            P("section", None, "head"),
            P("section", None, "head"),
            P("section", "head", None),
        ),
        out_specs=(P("rep", ("seq", "head"), "section"), P("section", "rep", "seq", None)),
        check_vma=False,
    )
```

```python
import functools

import jax
import jax.numpy as jnp
from jax import lax
from jax.experimental import pallas as pl
from jax.experimental.pallas import tpu as pltpu
from jax.sharding import PartitionSpec as P

HD = 128
MESH = pl.DeviceIdType.MESH
F32 = jnp.float32
BF16 = jnp.bfloat16


def rms_scale(values, gain):
    mean_sq = jnp.mean(values * values, axis=-1, keepdims=True)
    return values * lax.rsqrt(mean_sq + 1e-06) * gain


def dot_nt(a, b):
    return lax.dot_general(a, b, (((1,), (1,)), ((), ())), preferred_element_type=F32)


def kernel(
    dims,
    lengths_h,
    hidden,
    gain_h,
    lgain_h,
    wq,
    wl,
    wk,
    wv,
    wo,
    fin_v,
    lat_f,
    lengths,
    gain,
    lgain,
    hid_v,
    wq_v,
    wl_v,
    wk_v,
    wv_v,
    wo_v,
    x_s,
    normed_s,
    lat_b,
    cache,
    absorbed_s,
    attn_s,
    out_s,
    part_in,
    fin_in,
    load_sem,
    z_send,
    z_recv,
    h_send,
    h_recv,
    f_send,
    f_recv,
):
    seqs, sections, heads = dims
    seq = lax.axis_index("seq")
    sec = lax.axis_index("section")
    head = lax.axis_index("head")
    groups, rows, width = hid_v.shape
    rank = wl_v.shape[1]
    cols = wq_v.shape[1]
    heads_here = cols // HD
    share = rows // heads
    pw = width // sections
    tok = rows * seqs
    scale = 1.0 / HD**0.5
    sub = 2
    cw = pw // sub
    first_sec = sec == 0
    last_sec = sec == sections - 1

    loads = [
        pltpu.make_async_copy(src, dst, load_sem.at[i])
        for i, (src, dst) in enumerate(
            [
                (hidden, hid_v),
                (wl.at[0], wl_v),
                (wq.at[0], wq_v),
                (wk.at[0], wk_v),
                (wv.at[0], wv_v),
                (wo.at[0], wo_v),
            ]
        )
    ]
    small = [
        pltpu.make_async_copy(src, dst, load_sem.at[6 + i])
        for i, (src, dst) in enumerate([(gain_h, gain), (lgain_h, lgain), (lengths_h, lengths)])
    ]
    loads[0].start()
    for c in small:
        c.start()
    for c in loads[1:]:
        c.start()

    barrier = pltpu.get_barrier_semaphore()
    peers = [{"seq": lax.rem(seq + d, seqs)} for d in range(1, seqs)]
    for ds in range(sections):
        for dh in range(heads):
            if ds or dh:
                peers.append(
                    {
                        "section": lax.rem(sec + ds, sections),
                        "head": lax.rem(head + dh, heads),
                    }
                )
    for peer in peers:
        pl.semaphore_signal(barrier, inc=1, device_id=peer, device_id_type=MESH)

    own = pl.ds(pl.multiple_of(seq * rows, rows), rows)
    pos = seq * rows + lax.broadcasted_iota(jnp.int32, (rows, 1), 0)

    def z_copy(g, d):
        return pltpu.make_async_remote_copy(
            src_ref=lat_b.at[g],
            dst_ref=cache.at[(seq + d) // seqs, g, own],
            send_sem=z_send.at[g, d - 1],
            recv_sem=z_recv.at[g, d - 1],
            device_id={"seq": lax.rem(seq + d, seqs)},
            device_id_type=MESH,
        )

    def h_copy(g, p, dh):
        cols_p = pl.ds(p * cw, cw)
        return pltpu.make_async_remote_copy(
            src_ref=out_s.at[g, :, cols_p],
            dst_ref=part_in.at[head, g, :, cols_p],
            send_sem=h_send.at[g, p, dh],
            recv_sem=h_recv.at[g, p, head],
            device_id={"section": lax.rem(sec + 1, sections), "head": lax.rem(head + dh, heads)},
            device_id_type=MESH,
        )

    def h_arrival(g, p, source):
        cols_p = pl.ds(p * cw, cw)
        return pltpu.make_async_remote_copy(
            src_ref=out_s.at[g, :, cols_p],
            dst_ref=part_in.at[source, g, :, cols_p],
            send_sem=h_send.at[g, p, 0],
            recv_sem=h_recv.at[g, p, source],
            device_id={"section": lax.rem(sec + 1, sections)},
            device_id_type=MESH,
        )

    def f_copy(g, p, dh):
        to_head = lax.rem(head + dh, heads)
        return pltpu.make_async_remote_copy(
            src_ref=out_s.at[
                g, pl.ds(pl.multiple_of(to_head * share, share), share), pl.ds(p * cw, cw)
            ],
            dst_ref=fin_in.at[dh, g, :, pl.ds(p % sub * cw, cw)],
            send_sem=f_send.at[g, p, dh],
            recv_sem=f_recv.at[g, p % sub, dh],
            device_id={"section": p // sub, "head": to_head},
            device_id_type=MESH,
        )

    pairs = [
        (p, dh)
        for p in range(sections * sub)
        for dh in range(heads)
        if p // sub < sections - 1 or dh
    ]

    def latent_part(g0, ng):
        span = slice(g0 * rows, (g0 + ng) * rows)
        raw = jnp.dot(normed_s[span], wl_v[...], preferred_element_type=F32)
        full = rms_scale(raw, lgain[...])
        for i in range(ng):
            g = g0 + i
            piece = full[i * rows : (i + 1) * rows]
            narrow = piece.astype(BF16)
            lat_b[g] = narrow
            cache[0, g, own] = narrow
            lat_f[0, g] = jnp.where(pos < lengths[g], piece, 0.0)

    def latent_send(g):
        for d in range(seqs - 1, 0, -1):
            if g + 1 < groups:
                z_copy(g, d).start()
            else:

                @pl.when(seq + d < seqs)
                def _():
                    z_copy(g, d).start()

    def latents_below(g):
        for d in range(1, seqs):

            @pl.when(seq >= d)
            def _():
                z_copy(g, d).wait_recv()

    def latents_above(g):
        for d in range(seqs - 1, 0, -1):

            @pl.when(seq < d)
            def _():
                z_copy(g, d).wait_recv()
                at = pl.ds(pl.multiple_of((seq - d + seqs) * rows, rows), rows)
                cache[0, g, at] = cache[1, g, at]

    def query_part(g0, ng):
        span = slice(g0 * rows, (g0 + ng) * rows)
        query = jnp.dot(normed_s[span], wq_v[...], preferred_element_type=F32).astype(BF16)
        for h in range(heads_here):
            at = slice(h * HD, (h + 1) * HD)
            absorbed = (dot_nt(query[:, at], wk_v[:, at]) * scale).astype(BF16)
            for i in range(ng):
                absorbed_s[g0 + i, h * rows : (h + 1) * rows] = absorbed[i * rows : (i + 1) * rows]

    def take_input(g):
        for p in range(sections * sub):
            for source in range(heads):
                h_arrival(g, p, source).wait_recv()
        half = rows // 2
        for r0 in range(0, rows, half):
            r = slice(r0, r0 + half)
            added = part_in[0, g, r].astype(F32)
            for source in range(1, heads):
                added = added + part_in[source, g, r].astype(F32)
            x = hid_v[g, r].astype(F32) + added
            x_s[g, r] = x
            normed_s[g * rows + r0 : g * rows + r0 + half] = rms_scale(x, gain[...]).astype(BF16)

    def project_later(g):
        take_input(g)
        latent_part(g, 1)
        latent_send(g)
        query_part(g, 1)

    for d in range(1, seqs):

        @pl.when(seq + d < seqs)
        def _():
            at = pl.ds(pl.multiple_of((seq + d) * rows, rows), rows)
            for g in range(groups):
                cache[0, g, at] = jnp.zeros((rows, rank), BF16)

    loads[0].wait()
    for c in small:
        c.wait()

    @pl.when(first_sec)
    def _():
        half = rows // 2
        for g in range(groups):
            for r0 in range(0, rows, half):
                x = hid_v[g, r0 : r0 + half].astype(F32)
                if sections == 1:
                    x_s[g, r0 : r0 + half] = x
                normed_s[g * rows + r0 : g * rows + r0 + half] = rms_scale(x, gain[...]).astype(
                    BF16
                )
        loads[1].wait()
        latent_part(0, groups)

    pl.semaphore_wait(barrier, len(peers))

    @pl.when(first_sec)
    def _():
        for g in range(groups):
            latent_send(g)
        loads[2].wait()
        loads[3].wait()
        query_part(0, groups)

    @pl.when(jnp.logical_not(first_sec))
    def _():
        for i in range(1, 4):
            loads[i].wait()
        for g in range(min(2, groups)):
            project_later(g)

    loads[4].wait()
    loads[5].wait()

    key_pos = lax.broadcasted_iota(jnp.int32, (1, tok), 1)
    row_in = lax.broadcasted_iota(jnp.int32, (rows, 1), 0)
    mine = (row_in >= head * share) & (row_in < (head + 1) * share)

    def attend(g):
        keys = (g + 1) * tok
        per = heads_here
        while per > 2 and per * rows * keys > 512 * 768:
            per //= 2
        same = jnp.where(key_pos <= pos, 0.0, -1e30)
        same = jnp.concatenate([same] * per, axis=0)
        past = [jnp.where(key_pos < lengths[b], 0.0, -1e30) for b in range(g)]
        if g:
            latents_above(g - 1)
        latents_below(g)
        for h0 in range(0, heads_here, per):
            span = slice(h0 * rows, (h0 + per) * rows)
            scores = [dot_nt(absorbed_s[g, span], cache[0, b]) + past[b] for b in range(g)]
            scores.append(dot_nt(absorbed_s[g, span], cache[0, g]) + same)
            top = jnp.max(scores[0], axis=1, keepdims=True)
            for piece in scores[1:]:
                top = jnp.maximum(top, jnp.max(piece, axis=1, keepdims=True))
            total = None
            accum = None
            for b in range(g + 1):
                weights = jnp.exp(scores[b] - top)
                part = jnp.sum(weights, axis=1, keepdims=True)
                gained = jnp.dot(weights.astype(BF16), cache[0, b], preferred_element_type=F32)
                total = part if total is None else total + part
                accum = gained if accum is None else accum + gained
            context = (accum / total).astype(BF16)
            for i in range(0, per, 2):
                n = min(2, per - i)
                both = jnp.dot(
                    context[i * rows : (i + n) * rows],
                    wv_v[:, (h0 + i) * HD : (h0 + i + n) * HD],
                    preferred_element_type=F32,
                )
                for j in range(n):
                    at = slice((h0 + i + j) * HD, (h0 + i + j + 1) * HD)
                    attn_s[g, :, at] = both[
                        j * rows : (j + 1) * rows, j * HD : (j + 1) * HD
                    ].astype(BF16)

        @pl.when(jnp.logical_not(last_sec))
        def _():
            for p in range(sections * sub):
                at = slice(p * cw, (p + 1) * cw)
                out_s[g, :, at] = jnp.dot(
                    attn_s[g], wo_v[:, at], preferred_element_type=F32
                ).astype(BF16)
                for dh in range(heads - 1, -1, -1):
                    h_copy(g, p, dh).start()

        @pl.when(last_sec)
        def _():
            for p in range(sections * sub):
                at = slice(p * cw, (p + 1) * cw)
                added = jnp.dot(attn_s[g], wo_v[:, at], preferred_element_type=F32)
                state = x_s[g, :, at] + added
                x_s[g, :, at] = state
                out_s[g, :, at] = jnp.where(mine, state, added).astype(BF16)
                for dh in range(heads - 1, -1, -1):
                    if (p, dh) in pairs:
                        f_copy(g, p, dh).start()

    for g in range(groups):
        attend(g)
        if g + 2 < groups:

            @pl.when(jnp.logical_not(first_sec))
            def _():
                project_later(g + 2)

    out_pos = seq * rows + head * share + lax.broadcasted_iota(jnp.int32, (share, 1), 0)
    my_rows = pl.ds(pl.multiple_of(head * share, share), share)
    my_cols = pl.ds(pl.multiple_of(sec * pw, pw), pw)
    for g in range(groups):
        for q in range(sub):
            for dh in range(1, heads):
                f_copy(g, q, dh).wait_recv()

        @pl.when(last_sec)
        def _():
            fin_v[g] = x_s[g, my_rows, my_cols]

        @pl.when(jnp.logical_not(last_sec))
        def _():
            for q in range(sub):
                f_copy(g, q, 0).wait_recv()
            fin_v[g] = fin_in[0, g].astype(F32)

        value = fin_v[g]
        for dh in range(1, heads):
            value = value + fin_in[dh, g].astype(F32)
        fin_v[g] = jnp.where(out_pos < lengths[g], value, 0.0)

    for g in range(groups):
        for d in range(1, seqs):
            if g + 1 < groups:
                z_copy(g, d).wait_send()
            else:

                @pl.when(seq + d < seqs)
                def _():
                    z_copy(g, d).wait_send()

    @pl.when(jnp.logical_not(last_sec))
    def _():
        for g in range(groups):
            for p in range(sections * sub):
                for dh in range(heads):
                    h_copy(g, p, dh).wait_send()

    @pl.when(last_sec)
    def _():
        for g in range(groups):
            for p, dh in pairs:
                f_copy(g, p, dh).wait_send()


def solution(mesh):
    seqs, sections, heads = mesh.shape["seq"], mesh.shape["section"], mesh.shape["head"]

    def shards(hidden, lengths, attn_gain, w_query, w_latent, latent_gain, w_key, w_value, w_out):
        groups, rows, width = hidden.shape
        rank = w_latent.shape[2]
        cols = w_query.shape[2]
        share, pw = rows // heads, width // sections
        hbm = pl.BlockSpec(memory_space=pltpu.HBM)
        vmem = pl.BlockSpec(memory_space=pltpu.VMEM)
        dma = pltpu.SemaphoreType.DMA
        return pl.pallas_call(
            functools.partial(kernel, (seqs, sections, heads)),
            out_shape=(
                pltpu.VMEM((groups, share, pw), F32),
                pltpu.VMEM((1, groups, rows, rank), F32),
            ),
            in_specs=[hbm] * 9,
            out_specs=(vmem, vmem),
            scratch_shapes=[
                pltpu.SMEM((groups,), jnp.int32),
                pltpu.VMEM((1, width), F32),
                pltpu.VMEM((1, rank), F32),
                pltpu.VMEM((groups, rows, width), BF16),
                pltpu.VMEM((width, cols), BF16),
                pltpu.VMEM((width, rank), BF16),
                pltpu.VMEM((rank, cols), BF16),
                pltpu.VMEM((rank, cols), BF16),
                pltpu.VMEM((cols, width), BF16),
                pltpu.VMEM((groups, rows, width), F32),
                pltpu.VMEM((groups * rows, width), BF16),
                pltpu.VMEM((groups, rows, rank), BF16),
                pltpu.VMEM((2, groups, rows * seqs, rank), BF16),
                pltpu.VMEM((groups, cols // HD * rows, rank), BF16),
                pltpu.VMEM((groups, rows, cols), BF16),
                pltpu.VMEM((groups, rows, width), BF16),
                pltpu.VMEM((heads, groups, rows, width), BF16),
                pltpu.VMEM((heads, groups, share, pw), BF16),
                dma((9,)),
                dma((groups, max(1, seqs - 1))),
                dma((groups, max(1, seqs - 1))),
                dma((groups, 2 * sections, heads)),
                dma((groups, 2 * sections, heads)),
                dma((groups, 2 * sections, heads)),
                dma((groups, 2, heads)),
            ],
            compiler_params=pltpu.CompilerParams(
                collective_id=0, has_side_effects=True, vmem_limit_bytes=60 * 1024 * 1024
            ),
        )(lengths, hidden, attn_gain, latent_gain, w_query, w_latent, w_key, w_value, w_out)

    return jax.shard_map(
        shards,
        mesh=mesh,
        in_specs=(
            P("rep", "seq", None),
            P("rep"),
            P("section", None),
            P("section", None, "head"),
            P("section", None, None),
            P("section", None),
            P("section", None, "head"),
            P("section", None, "head"),
            P("section", "head", None),
        ),
        out_specs=(P("rep", ("seq", "head"), "section"), P("section", "rep", "seq", None)),
        check_vma=False,
    )
```

```python
import functools

import jax
import jax.numpy as jnp
from jax import lax
from jax.experimental import pallas as pl
from jax.experimental.pallas import tpu as pltpu
from jax.sharding import PartitionSpec as P

HD = 128
MESH = pl.DeviceIdType.MESH
F32 = jnp.float32
BF16 = jnp.bfloat16


def rms_scale(values, gain):
    mean_sq = jnp.mean(values * values, axis=-1, keepdims=True)
    return values * lax.rsqrt(mean_sq + 1e-06) * gain


def dot_nt(a, b):
    return lax.dot_general(a, b, (((1,), (1,)), ((), ())), preferred_element_type=F32)


def kernel(
    dims,
    lengths_h,
    hidden,
    gain_h,
    lgain_h,
    wq,
    wl,
    wk,
    wv,
    wo,
    fin_v,
    lat_f,
    lengths,
    gain,
    lgain,
    hid_v,
    wq_v,
    wl_v,
    wk_v,
    wk_t,
    wv_v,
    wo_v,
    x_s,
    normed_s,
    lat_b,
    cache,
    absorbed_s,
    attn_s,
    out_s,
    part_in,
    fin_in,
    load_sem,
    z_send,
    z_recv,
    h_send,
    h_recv,
    f_send,
    f_recv,
):
    seqs, sections, heads = dims
    seq = lax.axis_index("seq")
    sec = lax.axis_index("section")
    head = lax.axis_index("head")
    groups, rows, width = hid_v.shape
    rank = wl_v.shape[1]
    cols = wq_v.shape[1]
    heads_here = cols // HD
    share = rows // heads
    pw = width // sections
    tok = rows * seqs
    scale = 1.0 / HD**0.5
    sub = 2
    cw = pw // sub
    first_sec = sec == 0
    last_sec = sec == sections - 1

    loads = [
        pltpu.make_async_copy(src, dst, load_sem.at[i])
        for i, (src, dst) in enumerate(
            [
                (hidden, hid_v),
                (wl.at[0], wl_v),
                (wq.at[0], wq_v),
                (wk.at[0], wk_v),
                (wv.at[0], wv_v),
                (wo.at[0], wo_v),
            ]
        )
    ]
    small = [
        pltpu.make_async_copy(src, dst, load_sem.at[6 + i])
        for i, (src, dst) in enumerate([(gain_h, gain), (lgain_h, lgain), (lengths_h, lengths)])
    ]
    loads[0].start()
    for c in small:
        c.start()
    for c in loads[1:]:
        c.start()

    barrier = pltpu.get_barrier_semaphore()
    peers = [{"seq": lax.rem(seq + d, seqs)} for d in range(1, seqs)]
    for ds in range(sections):
        for dh in range(heads):
            if ds or dh:
                peers.append(
                    {
                        "section": lax.rem(sec + ds, sections),
                        "head": lax.rem(head + dh, heads),
                    }
                )
    for peer in peers:
        pl.semaphore_signal(barrier, inc=1, device_id=peer, device_id_type=MESH)

    own = pl.ds(pl.multiple_of(seq * rows, rows), rows)
    pos = seq * rows + lax.broadcasted_iota(jnp.int32, (rows, 1), 0)

    def z_copy(g, d):
        return pltpu.make_async_remote_copy(
            src_ref=lat_b.at[g],
            dst_ref=cache.at[(seq + d) // seqs, g, own],
            send_sem=z_send.at[g, d - 1],
            recv_sem=z_recv.at[g, d - 1],
            device_id={"seq": lax.rem(seq + d, seqs)},
            device_id_type=MESH,
        )

    def h_copy(g, p, dh):
        cols_p = pl.ds(p * cw, cw)
        return pltpu.make_async_remote_copy(
            src_ref=out_s.at[g, :, cols_p],
            dst_ref=part_in.at[head, g, :, cols_p],
            send_sem=h_send.at[g, p, dh],
            recv_sem=h_recv.at[g, p, head],
            device_id={"section": lax.rem(sec + 1, sections), "head": lax.rem(head + dh, heads)},
            device_id_type=MESH,
        )

    def h_arrival(g, p, source):
        cols_p = pl.ds(p * cw, cw)
        return pltpu.make_async_remote_copy(
            src_ref=out_s.at[g, :, cols_p],
            dst_ref=part_in.at[source, g, :, cols_p],
            send_sem=h_send.at[g, p, 0],
            recv_sem=h_recv.at[g, p, source],
            device_id={"section": lax.rem(sec + 1, sections)},
            device_id_type=MESH,
        )

    def f_copy(g, p, dh):
        to_head = lax.rem(head + dh, heads)
        return pltpu.make_async_remote_copy(
            src_ref=out_s.at[
                g, pl.ds(pl.multiple_of(to_head * share, share), share), pl.ds(p * cw, cw)
            ],
            dst_ref=fin_in.at[dh, g, :, pl.ds(p % sub * cw, cw)],
            send_sem=f_send.at[g, p, dh],
            recv_sem=f_recv.at[g, p % sub, dh],
            device_id={"section": p // sub, "head": to_head},
            device_id_type=MESH,
        )

    pairs = [
        (p, dh)
        for p in range(sections * sub)
        for dh in range(heads)
        if p // sub < sections - 1 or dh
    ]

    def latent_part(g0, ng):
        span = slice(g0 * rows, (g0 + ng) * rows)
        raw = jnp.dot(normed_s[span], wl_v[...], preferred_element_type=F32)
        full = rms_scale(raw, lgain[...])
        for i in range(ng):
            g = g0 + i
            piece = full[i * rows : (i + 1) * rows]
            narrow = piece.astype(BF16)
            lat_b[g] = narrow
            cache[0, g, own] = narrow
            lat_f[0, g] = jnp.where(pos < lengths[g], piece, 0.0)

    def latent_send(g):
        for d in range(seqs - 1, 0, -1):
            z_copy(g, d).start()

    def latents_below(g):
        for d in range(1, seqs):

            @pl.when(seq >= d)
            def _():
                z_copy(g, d).wait_recv()

    def latents_above(g):
        for d in range(seqs - 1, 0, -1):

            @pl.when(seq < d)
            def _():
                z_copy(g, d).wait_recv()
                at = pl.ds(pl.multiple_of((seq - d + seqs) * rows, rows), rows)
                cache[0, g, at] = cache[1, g, at]

    def query_part(g0, ng, keys_t):
        span = slice(g0 * rows, (g0 + ng) * rows)
        query = jnp.dot(normed_s[span], wq_v[...], preferred_element_type=F32).astype(BF16)
        for h in range(heads_here):
            at = slice(h * HD, (h + 1) * HD)
            if keys_t is None:
                absorbed = dot_nt(query[:, at], wk_v[:, at])
            else:
                absorbed = jnp.dot(query[:, at], keys_t[at], preferred_element_type=F32)
            absorbed = (absorbed * scale).astype(BF16)
            for i in range(ng):
                absorbed_s[g0 + i, h * rows : (h + 1) * rows] = absorbed[i * rows : (i + 1) * rows]

    def take_input(g):
        for p in range(sections * sub):
            for source in range(heads):
                h_arrival(g, p, source).wait_recv()
        half = rows // 2
        for r0 in range(0, rows, half):
            r = slice(r0, r0 + half)
            added = part_in[0, g, r].astype(F32)
            for source in range(1, heads):
                added = added + part_in[source, g, r].astype(F32)
            x = hid_v[g, r].astype(F32) + added
            x_s[g, r] = x
            normed_s[g * rows + r0 : g * rows + r0 + half] = rms_scale(x, gain[...]).astype(BF16)

    def project_later(g):
        take_input(g)
        latent_part(g, 1)
        latent_send(g)
        query_part(g, 1, wk_t)

    for d in range(1, seqs):

        @pl.when(seq + d < seqs)
        def _():
            at = pl.ds(pl.multiple_of((seq + d) * rows, rows), rows)
            for g in range(groups):
                cache[0, g, at] = jnp.zeros((rows, rank), BF16)

    loads[0].wait()
    for c in small:
        c.wait()

    @pl.when(first_sec)
    def _():
        half = rows // 2
        for g in range(groups):
            for r0 in range(0, rows, half):
                x = hid_v[g, r0 : r0 + half].astype(F32)
                normed_s[g * rows + r0 : g * rows + r0 + half] = rms_scale(x, gain[...]).astype(
                    BF16
                )
        loads[1].wait()
        latent_part(0, groups)

    pl.semaphore_wait(barrier, len(peers))

    key_pos = lax.broadcasted_iota(jnp.int32, (1, tok), 1)
    row_in = lax.broadcasted_iota(jnp.int32, (rows, 1), 0)
    mine = (row_in >= head * share) & (row_in < (head + 1) * share)

    def attend(g, last):
        keys = (g + 1) * tok
        per = heads_here
        while per > 2 and per * rows * keys > 512 * 768:
            per //= 2
        same = jnp.where(key_pos <= pos, 0.0, -1e30)
        same = jnp.concatenate([same] * per, axis=0)
        past = [jnp.where(key_pos < lengths[b], 0.0, -1e30) for b in range(g)]
        if g:
            latents_above(g - 1)
        latents_below(g)
        for h0 in range(0, heads_here, per):
            span = slice(h0 * rows, (h0 + per) * rows)
            scores = [dot_nt(absorbed_s[g, span], cache[0, b]) + past[b] for b in range(g)]
            scores.append(dot_nt(absorbed_s[g, span], cache[0, g]) + same)
            top = scores[0]
            for piece in scores[1:]:
                top = jnp.maximum(top, piece)
            top = jnp.max(top, axis=1, keepdims=True)
            total = None
            accum = None
            for b in range(g + 1):
                weights = jnp.exp(scores[b] - top)
                gained = jnp.dot(weights.astype(BF16), cache[0, b], preferred_element_type=F32)
                total = weights if total is None else total + weights
                accum = gained if accum is None else accum + gained
            total = jnp.sum(total, axis=1, keepdims=True)
            context = (accum / total).astype(BF16)
            for i in range(0, per, 2):
                n = min(2, per - i)
                both = jnp.dot(
                    context[i * rows : (i + n) * rows],
                    wv_v[:, (h0 + i) * HD : (h0 + i + n) * HD],
                    preferred_element_type=F32,
                )
                for j in range(n):
                    at = slice((h0 + i + j) * HD, (h0 + i + j + 1) * HD)
                    attn_s[g, :, at] = both[
                        j * rows : (j + 1) * rows, j * HD : (j + 1) * HD
                    ].astype(BF16)

        for p in range(sections * sub):
            at = slice(p * cw, (p + 1) * cw)
            added = jnp.dot(attn_s[g], wo_v[:, at], preferred_element_type=F32)
            if last:
                state = x_s[g, :, at] + added
                x_s[g, :, at] = state
                added = jnp.where(mine, state, added)
            out_s[g, :, at] = added.astype(BF16)
            for dh in range(heads - 1, -1, -1):
                if not last:
                    h_copy(g, p, dh).start()
                elif (p, dh) in pairs:
                    f_copy(g, p, dh).start()

    @pl.when(first_sec)
    def _():
        for g in range(groups):
            latent_send(g)
        loads[2].wait()
        loads[3].wait()
        query_part(0, groups, None)
        loads[4].wait()
        loads[5].wait()
        for g in range(groups):
            attend(g, False)

    @pl.when(jnp.logical_not(first_sec))
    def _():
        for c in loads[1:]:
            c.wait()
        wk_t[...] = wk_v[...].T
        for g in range(min(2, groups)):
            project_later(g)
        for g in range(groups):
            attend(g, True)
            if g + 2 < groups:
                project_later(g + 2)

    out_pos = seq * rows + head * share + lax.broadcasted_iota(jnp.int32, (share, 1), 0)
    my_rows = pl.ds(pl.multiple_of(head * share, share), share)
    my_cols = pl.ds(pl.multiple_of(sec * pw, pw), pw)
    for g in range(groups):
        for q in range(sub):
            for dh in range(1, heads):
                f_copy(g, q, dh).wait_recv()

        @pl.when(last_sec)
        def _():
            fin_v[g] = x_s[g, my_rows, my_cols]

        @pl.when(jnp.logical_not(last_sec))
        def _():
            for q in range(sub):
                f_copy(g, q, 0).wait_recv()
            fin_v[g] = fin_in[0, g].astype(F32)

        value = fin_v[g]
        for dh in range(1, heads):
            value = value + fin_in[dh, g].astype(F32)
        fin_v[g] = jnp.where(out_pos < lengths[g], value, 0.0)

    for g in range(groups):
        for d in range(1, seqs):
            z_copy(g, d).wait_send()
    for d in range(1, seqs):

        @pl.when(seq < d)
        def _():
            z_copy(groups - 1, d).wait_recv()

    @pl.when(jnp.logical_not(last_sec))
    def _():
        for g in range(groups):
            for p in range(sections * sub):
                for dh in range(heads):
                    h_copy(g, p, dh).wait_send()

    @pl.when(last_sec)
    def _():
        for g in range(groups):
            for p, dh in pairs:
                f_copy(g, p, dh).wait_send()


def flush(final_v, latents_v, final, latents, sem):
    copies = [
        pltpu.make_async_copy(final_v, final, sem.at[0]),
        pltpu.make_async_copy(latents_v, latents, sem.at[1]),
    ]
    for c in copies:
        c.start()
    for c in copies:
        c.wait()


def solution(mesh):
    seqs, sections, heads = mesh.shape["seq"], mesh.shape["section"], mesh.shape["head"]

    def shards(hidden, lengths, attn_gain, w_query, w_latent, latent_gain, w_key, w_value, w_out):
        groups, rows, width = hidden.shape
        rank = w_latent.shape[2]
        cols = w_query.shape[2]
        share, pw = rows // heads, width // sections
        hbm = pl.BlockSpec(memory_space=pltpu.HBM)
        vmem = pl.BlockSpec(memory_space=pltpu.VMEM)
        dma = pltpu.SemaphoreType.DMA
        final_v, latents_v = pl.pallas_call(
            functools.partial(kernel, (seqs, sections, heads)),
            out_shape=(
                pltpu.VMEM((groups, share, pw), F32),
                pltpu.VMEM((1, groups, rows, rank), F32),
            ),
            in_specs=[hbm] * 9,
            out_specs=(vmem, vmem),
            scratch_shapes=[
                pltpu.SMEM((groups,), jnp.int32),
                pltpu.VMEM((1, width), F32),
                pltpu.VMEM((1, rank), F32),
                pltpu.VMEM((groups, rows, width), BF16),
                pltpu.VMEM((width, cols), BF16),
                pltpu.VMEM((width, rank), BF16),
                pltpu.VMEM((rank, cols), BF16),
                pltpu.VMEM((cols, rank), BF16),
                pltpu.VMEM((rank, cols), BF16),
                pltpu.VMEM((cols, width), BF16),
                pltpu.VMEM((groups, rows, width), F32),
                pltpu.VMEM((groups * rows, width), BF16),
                pltpu.VMEM((groups, rows, rank), BF16),
                pltpu.VMEM((2, groups, rows * seqs, rank), BF16),
                pltpu.VMEM((groups, cols // HD * rows, rank), BF16),
                pltpu.VMEM((groups, rows, cols), BF16),
                pltpu.VMEM((groups, rows, width), BF16),
                pltpu.VMEM((heads, groups, rows, width), BF16),
                pltpu.VMEM((heads, groups, share, pw), BF16),
                dma((9,)),
                dma((groups, max(1, seqs - 1))),
                dma((groups, max(1, seqs - 1))),
                dma((groups, 2 * sections, heads)),
                dma((groups, 2 * sections, heads)),
                dma((groups, 2 * sections, heads)),
                dma((groups, 2, heads)),
            ],
            compiler_params=pltpu.CompilerParams(
                collective_id=0, has_side_effects=True, vmem_limit_bytes=60 * 1024 * 1024
            ),
        )(lengths, hidden, attn_gain, latent_gain, w_query, w_latent, w_key, w_value, w_out)
        return pl.pallas_call(
            flush,
            out_shape=(
                jax.ShapeDtypeStruct(final_v.shape, F32),
                jax.ShapeDtypeStruct(latents_v.shape, F32),
            ),
            in_specs=[vmem] * 2,
            out_specs=(hbm, hbm),
            scratch_shapes=[dma((2,))],
            compiler_params=pltpu.CompilerParams(vmem_limit_bytes=1024 * 1024),
        )(final_v, latents_v)

    return jax.shard_map(
        shards,
        mesh=mesh,
        in_specs=(
            P("rep", "seq", None),
            P("rep"),
            P("section", None),
            P("section", None, "head"),
            P("section", None, None),
            P("section", None),
            P("section", None, "head"),
            P("section", None, "head"),
            P("section", "head", None),
        ),
        out_specs=(P("rep", ("seq", "head"), "section"), P("section", "rep", "seq", None)),
        check_vma=False,
    )
```

```python
import functools

import jax
import jax.numpy as jnp
from jax import lax
from jax.experimental import pallas as pl
from jax.experimental.pallas import tpu as pltpu
from jax.sharding import PartitionSpec as P

HD = 128
MESH = pl.DeviceIdType.MESH
F32 = jnp.float32
BF16 = jnp.bfloat16


def rms_scale(values, gain):
    mean_sq = jnp.mean(values * values, axis=-1, keepdims=True)
    return values * lax.rsqrt(mean_sq + 1e-06) * gain


def dot_nt(a, b):
    return lax.dot_general(a, b, (((1,), (1,)), ((), ())), preferred_element_type=F32)


def kernel(
    dims,
    lengths_h,
    hidden,
    gain_h,
    lgain_h,
    wq,
    wl,
    wk,
    wv,
    wo,
    fin_v,
    lat_f,
    lengths,
    gain,
    lgain,
    hid_v,
    wq_v,
    wl_v,
    wk_v,
    wk_t,
    wv_v,
    wo_v,
    x_s,
    normed_s,
    lat_b,
    cache,
    absorbed_s,
    attn_s,
    out_s,
    part_in,
    fin_in,
    weights_s,
    load_sem,
    z_send,
    z_recv,
    h_send,
    h_recv,
    f_send,
    f_recv,
):
    seqs, sections, heads = dims
    seq = lax.axis_index("seq")
    sec = lax.axis_index("section")
    head = lax.axis_index("head")
    groups, rows, width = hid_v.shape
    rank = wl_v.shape[1]
    cols = wq_v.shape[1]
    heads_here = cols // HD
    share = rows // heads
    pw = width // sections
    tok = rows * seqs
    scale = 1.0 / HD**0.5
    sub = 2
    cw = pw // sub
    first_sec = sec == 0
    last_sec = sec == sections - 1

    loads = [
        pltpu.make_async_copy(src, dst, load_sem.at[i])
        for i, (src, dst) in enumerate(
            [
                (hidden, hid_v),
                (wl.at[0], wl_v),
                (wq.at[0], wq_v),
                (wk.at[0], wk_v),
                (wv.at[0], wv_v),
                (wo.at[0], wo_v),
            ]
        )
    ]
    small = [
        pltpu.make_async_copy(src, dst, load_sem.at[6 + i])
        for i, (src, dst) in enumerate([(gain_h, gain), (lgain_h, lgain), (lengths_h, lengths)])
    ]
    loads[0].start()
    for c in small:
        c.start()
    for c in loads[1:]:
        c.start()

    barrier = pltpu.get_barrier_semaphore()
    peers = [{"seq": lax.rem(seq + d, seqs)} for d in range(1, seqs)]
    for ds in range(sections):
        for dh in range(heads):
            if ds or dh:
                peers.append(
                    {
                        "section": lax.rem(sec + ds, sections),
                        "head": lax.rem(head + dh, heads),
                    }
                )
    for peer in peers:
        pl.semaphore_signal(barrier, inc=1, device_id=peer, device_id_type=MESH)

    own = pl.ds(pl.multiple_of(seq * rows, rows), rows)
    pos = seq * rows + lax.broadcasted_iota(jnp.int32, (rows, 1), 0)

    def z_copy(g, d):
        return pltpu.make_async_remote_copy(
            src_ref=lat_b.at[g],
            dst_ref=cache.at[(seq + d) // seqs, g, own],
            send_sem=z_send.at[g, d - 1],
            recv_sem=z_recv.at[g, d - 1],
            device_id={"seq": lax.rem(seq + d, seqs)},
            device_id_type=MESH,
        )

    def h_copy(g, p, dh):
        cols_p = pl.ds(p * cw, cw)
        return pltpu.make_async_remote_copy(
            src_ref=out_s.at[g, :, cols_p],
            dst_ref=part_in.at[head, g, :, cols_p],
            send_sem=h_send.at[g, p, dh],
            recv_sem=h_recv.at[g, p, head],
            device_id={"section": lax.rem(sec + 1, sections), "head": lax.rem(head + dh, heads)},
            device_id_type=MESH,
        )

    def h_arrival(g, p, source):
        cols_p = pl.ds(p * cw, cw)
        return pltpu.make_async_remote_copy(
            src_ref=out_s.at[g, :, cols_p],
            dst_ref=part_in.at[source, g, :, cols_p],
            send_sem=h_send.at[g, p, 0],
            recv_sem=h_recv.at[g, p, source],
            device_id={"section": lax.rem(sec + 1, sections)},
            device_id_type=MESH,
        )

    def f_copy(g, p, dh):
        to_head = lax.rem(head + dh, heads)
        return pltpu.make_async_remote_copy(
            src_ref=out_s.at[
                g, pl.ds(pl.multiple_of(to_head * share, share), share), pl.ds(p * cw, cw)
            ],
            dst_ref=fin_in.at[dh, g, :, pl.ds(p % sub * cw, cw)],
            send_sem=f_send.at[g, p, dh],
            recv_sem=f_recv.at[g, p % sub, dh],
            device_id={"section": p // sub, "head": to_head},
            device_id_type=MESH,
        )

    pairs = [
        (p, dh)
        for p in range(sections * sub)
        for dh in range(heads)
        if p // sub < sections - 1 or dh
    ]

    def latent_part(g0, ng):
        span = slice(g0 * rows, (g0 + ng) * rows)
        raw = jnp.dot(normed_s[span], wl_v[...], preferred_element_type=F32)
        full = rms_scale(raw, lgain[...])
        for i in range(ng):
            g = g0 + i
            piece = full[i * rows : (i + 1) * rows]
            narrow = piece.astype(BF16)
            lat_b[g] = narrow
            cache[0, g, own] = narrow
            lat_f[0, g] = jnp.where(pos < lengths[g], piece, 0.0)

    def latent_send(g):
        for d in range(1, seqs):
            z_copy(g, d).start()

    def latents_below(g):
        for d in range(1, seqs):

            @pl.when(seq >= d)
            def _():
                z_copy(g, d).wait_recv()

    def latents_above(g):
        for d in range(seqs - 1, 0, -1):

            @pl.when(seq < d)
            def _():
                z_copy(g, d).wait_recv()
                at = pl.ds(pl.multiple_of((seq - d + seqs) * rows, rows), rows)
                cache[0, g, at] = cache[1, g, at]

    def query_part(g0, ng, keys_t):
        span = slice(g0 * rows, (g0 + ng) * rows)
        query = jnp.dot(normed_s[span], wq_v[...], preferred_element_type=F32).astype(BF16)
        for h in range(heads_here):
            at = slice(h * HD, (h + 1) * HD)
            if keys_t is None:
                absorbed = dot_nt(query[:, at], wk_v[:, at])
            else:
                absorbed = jnp.dot(query[:, at], keys_t[at], preferred_element_type=F32)
            absorbed = (absorbed * scale).astype(BF16)
            for i in range(ng):
                absorbed_s[g0 + i, h * rows : (h + 1) * rows] = absorbed[i * rows : (i + 1) * rows]

    def take_input(g):
        for p in range(sections * sub):
            for source in range(heads):
                h_arrival(g, p, source).wait_recv()
        half = rows // 2
        for r0 in range(0, rows, half):
            r = slice(r0, r0 + half)
            added = part_in[0, g, r].astype(F32)
            for source in range(1, heads):
                added = added + part_in[source, g, r].astype(F32)
            x = hid_v[g, r].astype(F32) + added
            x_s[g, r] = x
            normed_s[g * rows + r0 : g * rows + r0 + half] = rms_scale(x, gain[...]).astype(BF16)

    def project_later(g):
        take_input(g)
        latent_part(g, 1)
        latent_send(g)
        query_part(g, 1, wk_t)

    for d in range(1, seqs):

        @pl.when(seq + d < seqs)
        def _():
            at = pl.ds(pl.multiple_of((seq + d) * rows, rows), rows)
            for g in range(groups):
                cache[0, g, at] = jnp.zeros((rows, rank), BF16)

    loads[0].wait()
    for c in small:
        c.wait()

    @pl.when(first_sec)
    def _():
        half = rows // 2
        for g in range(groups):
            for r0 in range(0, rows, half):
                x = hid_v[g, r0 : r0 + half].astype(F32)
                normed_s[g * rows + r0 : g * rows + r0 + half] = rms_scale(x, gain[...]).astype(
                    BF16
                )
        loads[1].wait()
        latent_part(0, groups)

    pl.semaphore_wait(barrier, len(peers))

    key_pos = lax.broadcasted_iota(jnp.int32, (1, tok), 1)
    row_in = lax.broadcasted_iota(jnp.int32, (rows, 1), 0)
    mine = (row_in >= head * share) & (row_in < (head + 1) * share)

    def attend(g, last):
        keys = (g + 1) * tok
        per = heads_here
        while per > 2 and per * rows * keys > 512 * 768:
            per //= 2
        same = jnp.where(key_pos <= pos, 0.0, -1e30)
        same = jnp.concatenate([same] * per, axis=0)
        past = [jnp.where(key_pos < lengths[b], 0.0, -1e30) for b in range(g)]
        if g:
            latents_above(g - 1)
        latents_below(g)
        for h0 in range(0, heads_here, per):
            span = slice(h0 * rows, (h0 + per) * rows)
            scores = [dot_nt(absorbed_s[g, span], cache[0, b]) + past[b] for b in range(g)]
            scores.append(dot_nt(absorbed_s[g, span], cache[0, g]) + same)
            top = scores[0]
            for piece in scores[1:]:
                top = jnp.maximum(top, piece)
            top = jnp.max(top, axis=1, keepdims=True)
            total = None
            for b in range(g + 1):
                weights = jnp.exp(scores[b] - top)
                total = weights if total is None else total + weights
                weights_s[: per * rows, b * tok : (b + 1) * tok] = weights.astype(BF16)
            total = jnp.sum(total, axis=1, keepdims=True)
            accum = jnp.dot(
                weights_s[: per * rows, :keys],
                cache[0, : g + 1].reshape(keys, rank),
                preferred_element_type=F32,
            )
            context = (accum / total).astype(BF16)
            for i in range(0, per, 2):
                n = min(2, per - i)
                both = jnp.dot(
                    context[i * rows : (i + n) * rows],
                    wv_v[:, (h0 + i) * HD : (h0 + i + n) * HD],
                    preferred_element_type=F32,
                )
                for j in range(n):
                    at = slice((h0 + i + j) * HD, (h0 + i + j + 1) * HD)
                    attn_s[g, :, at] = both[
                        j * rows : (j + 1) * rows, j * HD : (j + 1) * HD
                    ].astype(BF16)

        for p in range(sections * sub):
            at = slice(p * cw, (p + 1) * cw)
            added = jnp.dot(attn_s[g], wo_v[:, at], preferred_element_type=F32)
            if last:
                state = x_s[g, :, at] + added
                x_s[g, :, at] = state
                added = jnp.where(mine, state, added)
            out_s[g, :, at] = added.astype(BF16)
            for dh in range(heads - 1, -1, -1):
                if not last:
                    h_copy(g, p, dh).start()
                elif (p, dh) in pairs:
                    f_copy(g, p, dh).start()

    @pl.when(first_sec)
    def _():
        for g in range(groups):
            for d in range(1, seqs):
                z_copy(g, d).start()
        loads[2].wait()
        loads[3].wait()
        query_part(0, groups, None)
        loads[4].wait()
        loads[5].wait()
        for g in range(groups):
            attend(g, False)

    @pl.when(jnp.logical_not(first_sec))
    def _():
        for c in loads[1:]:
            c.wait()
        wk_t[...] = wk_v[...].T
        for g in range(min(2, groups)):
            project_later(g)
        for g in range(groups):
            attend(g, True)
            if g + 2 < groups:
                project_later(g + 2)

    out_pos = seq * rows + head * share + lax.broadcasted_iota(jnp.int32, (share, 1), 0)
    my_rows = pl.ds(pl.multiple_of(head * share, share), share)
    my_cols = pl.ds(pl.multiple_of(sec * pw, pw), pw)
    for g in range(groups):
        for q in range(sub):
            for dh in range(1, heads):
                f_copy(g, q, dh).wait_recv()

        @pl.when(last_sec)
        def _():
            fin_v[g] = x_s[g, my_rows, my_cols]

        @pl.when(jnp.logical_not(last_sec))
        def _():
            for q in range(sub):
                f_copy(g, q, 0).wait_recv()
            fin_v[g] = fin_in[0, g].astype(F32)

        value = fin_v[g]
        for dh in range(1, heads):
            value = value + fin_in[dh, g].astype(F32)
        fin_v[g] = jnp.where(out_pos < lengths[g], value, 0.0)

    for g in range(groups):
        for d in range(1, seqs):
            z_copy(g, d).wait_send()
    for d in range(1, seqs):

        @pl.when(seq < d)
        def _():
            z_copy(groups - 1, d).wait_recv()

    @pl.when(jnp.logical_not(last_sec))
    def _():
        for g in range(groups):
            for p in range(sections * sub):
                for dh in range(heads):
                    h_copy(g, p, dh).wait_send()

    @pl.when(last_sec)
    def _():
        for g in range(groups):
            for p, dh in pairs:
                f_copy(g, p, dh).wait_send()


def flush(final_v, latents_v, final, latents, sem):
    copies = [
        pltpu.make_async_copy(final_v, final, sem.at[0]),
        pltpu.make_async_copy(latents_v, latents, sem.at[1]),
    ]
    for c in copies:
        c.start()
    for c in copies:
        c.wait()


def solution(mesh):
    seqs, sections, heads = mesh.shape["seq"], mesh.shape["section"], mesh.shape["head"]

    def shards(hidden, lengths, attn_gain, w_query, w_latent, latent_gain, w_key, w_value, w_out):
        groups, rows, width = hidden.shape
        rank = w_latent.shape[2]
        cols = w_query.shape[2]
        share, pw = rows // heads, width // sections
        hbm = pl.BlockSpec(memory_space=pltpu.HBM)
        vmem = pl.BlockSpec(memory_space=pltpu.VMEM)
        dma = pltpu.SemaphoreType.DMA
        final_v, latents_v = pl.pallas_call(
            functools.partial(kernel, (seqs, sections, heads)),
            out_shape=(
                pltpu.VMEM((groups, share, pw), F32),
                pltpu.VMEM((1, groups, rows, rank), F32),
            ),
            in_specs=[hbm] * 9,
            out_specs=(vmem, vmem),
            scratch_shapes=[
                pltpu.SMEM((groups,), jnp.int32),
                pltpu.VMEM((1, width), F32),
                pltpu.VMEM((1, rank), F32),
                pltpu.VMEM((groups, rows, width), BF16),
                pltpu.VMEM((width, cols), BF16),
                pltpu.VMEM((width, rank), BF16),
                pltpu.VMEM((rank, cols), BF16),
                pltpu.VMEM((cols, rank), BF16),
                pltpu.VMEM((rank, cols), BF16),
                pltpu.VMEM((cols, width), BF16),
                pltpu.VMEM((groups, rows, width), F32),
                pltpu.VMEM((groups * rows, width), BF16),
                pltpu.VMEM((groups, rows, rank), BF16),
                pltpu.VMEM((2, groups, rows * seqs, rank), BF16),
                pltpu.VMEM((groups, cols // HD * rows, rank), BF16),
                pltpu.VMEM((groups, rows, cols), BF16),
                pltpu.VMEM((groups, rows, width), BF16),
                pltpu.VMEM((heads, groups, rows, width), BF16),
                pltpu.VMEM((heads, groups, share, pw), BF16),
                pltpu.VMEM((cols // HD * rows, groups * rows * seqs), BF16),
                dma((9,)),
                dma((groups, max(1, seqs - 1))),
                dma((groups, max(1, seqs - 1))),
                dma((groups, 2 * sections, heads)),
                dma((groups, 2 * sections, heads)),
                dma((groups, 2 * sections, heads)),
                dma((groups, 2, heads)),
            ],
            compiler_params=pltpu.CompilerParams(
                collective_id=0, has_side_effects=True, vmem_limit_bytes=60 * 1024 * 1024
            ),
        )(lengths, hidden, attn_gain, latent_gain, w_query, w_latent, w_key, w_value, w_out)
        return pl.pallas_call(
            flush,
            out_shape=(
                jax.ShapeDtypeStruct(final_v.shape, F32),
                jax.ShapeDtypeStruct(latents_v.shape, F32),
            ),
            in_specs=[vmem] * 2,
            out_specs=(hbm, hbm),
            scratch_shapes=[dma((2,))],
            compiler_params=pltpu.CompilerParams(vmem_limit_bytes=1024 * 1024),
        )(final_v, latents_v)

    return jax.shard_map(
        shards,
        mesh=mesh,
        in_specs=(
            P("rep", "seq", None),
            P("rep"),
            P("section", None),
            P("section", None, "head"),
            P("section", None, None),
            P("section", None),
            P("section", None, "head"),
            P("section", None, "head"),
            P("section", "head", None),
        ),
        out_specs=(P("rep", ("seq", "head"), "section"), P("section", "rep", "seq", None)),
        check_vma=False,
    )
```

```python
import functools

import jax
import jax.numpy as jnp
from jax import lax
from jax.experimental import pallas as pl
from jax.experimental.pallas import tpu as pltpu
from jax.sharding import PartitionSpec as P

HD = 128
MESH = pl.DeviceIdType.MESH
F32 = jnp.float32
BF16 = jnp.bfloat16


def rms_scale(values, gain):
    mean_sq = jnp.mean(values * values, axis=-1, keepdims=True)
    return values * lax.rsqrt(mean_sq + 1e-06) * gain


def dot_nt(a, b):
    return lax.dot_general(a, b, (((1,), (1,)), ((), ())), preferred_element_type=F32)


def kernel(
    dims,
    lengths_h,
    hidden,
    gain_h,
    lgain_h,
    wq,
    wl,
    wk,
    wv,
    wo,
    fin_v,
    lat_f,
    lengths,
    gain,
    lgain,
    hid_v,
    wq_v,
    wl_v,
    wk_v,
    wk_t,
    wv_v,
    wo_v,
    x_s,
    normed_s,
    lat_b,
    cache,
    absorbed_s,
    attn_s,
    out_s,
    part_in,
    fin_in,
    weights_s,
    load_sem,
    z_send,
    z_recv,
    o_send,
    h_recv,
    f_recv,
):
    seqs, sections, heads = dims
    seq = lax.axis_index("seq")
    sec = lax.axis_index("section")
    head = lax.axis_index("head")
    groups, rows, width = hid_v.shape
    rank = wl_v.shape[1]
    cols = wq_v.shape[1]
    heads_here = cols // HD
    share = rows // heads
    pw = width // sections
    tok = rows * seqs
    scale = 1.0 / HD**0.5
    sub = 2
    cw = pw // sub
    first_sec = sec == 0
    last_sec = sec == sections - 1

    loads = [
        pltpu.make_async_copy(src, dst, load_sem.at[i])
        for i, (src, dst) in enumerate(
            [
                (hidden, hid_v),
                (wl.at[0], wl_v),
                (wq.at[0], wq_v),
                (wk.at[0], wk_v),
                (wv.at[0], wv_v),
                (wo.at[0], wo_v),
            ]
        )
    ]
    small = [
        pltpu.make_async_copy(src, dst, load_sem.at[6 + i])
        for i, (src, dst) in enumerate([(gain_h, gain), (lgain_h, lgain), (lengths_h, lengths)])
    ]
    loads[0].start()
    for c in small:
        c.start()
    for c in loads[1:]:
        c.start()

    barrier = pltpu.get_barrier_semaphore()
    peers = [{"seq": lax.rem(seq + d, seqs)} for d in range(1, seqs)]
    for ds in range(sections):
        for dh in range(heads):
            if ds or dh:
                peers.append(
                    {
                        "section": lax.rem(sec + ds, sections),
                        "head": lax.rem(head + dh, heads),
                    }
                )
    for peer in peers:
        pl.semaphore_signal(barrier, inc=1, device_id=peer, device_id_type=MESH)

    own = pl.ds(pl.multiple_of(seq * rows, rows), rows)
    pos = seq * rows + lax.broadcasted_iota(jnp.int32, (rows, 1), 0)

    def z_copy(g, d):
        return pltpu.make_async_remote_copy(
            src_ref=lat_b.at[g],
            dst_ref=cache.at[(seq + d) // seqs, g, own],
            send_sem=z_send.at[0],
            recv_sem=z_recv.at[g, d - 1],
            device_id={"seq": lax.rem(seq + d, seqs)},
            device_id_type=MESH,
        )

    def h_copy(g, p, dh):
        cols_p = pl.ds(p * cw, cw)
        return pltpu.make_async_remote_copy(
            src_ref=out_s.at[g, :, cols_p],
            dst_ref=part_in.at[head, g, :, cols_p],
            send_sem=o_send.at[0],
            recv_sem=h_recv.at[g],
            device_id={"section": lax.rem(sec + 1, sections), "head": lax.rem(head + dh, heads)},
            device_id_type=MESH,
        )

    def waiter(ref, sem):
        return pltpu.make_async_remote_copy(
            src_ref=ref,
            dst_ref=ref,
            send_sem=sem,
            recv_sem=sem,
            device_id={"section": lax.rem(sec + 1, sections)},
            device_id_type=MESH,
        )

    def f_copy(g, p, dh):
        to_head = lax.rem(head + dh, heads)
        return pltpu.make_async_remote_copy(
            src_ref=out_s.at[
                g, pl.ds(pl.multiple_of(to_head * share, share), share), pl.ds(p * cw, cw)
            ],
            dst_ref=fin_in.at[dh, g, :, pl.ds(p % sub * cw, cw)],
            send_sem=o_send.at[0],
            recv_sem=f_recv.at[g],
            device_id={"section": p // sub, "head": to_head},
            device_id_type=MESH,
        )

    pairs = [
        (p, dh)
        for p in range(sections * sub)
        for dh in range(heads)
        if p // sub < sections - 1 or dh
    ]

    def latent_part(g0, ng):
        span = slice(g0 * rows, (g0 + ng) * rows)
        raw = jnp.dot(normed_s[span], wl_v[...], preferred_element_type=F32)
        full = rms_scale(raw, lgain[...])
        for i in range(ng):
            g = g0 + i
            piece = full[i * rows : (i + 1) * rows]
            narrow = piece.astype(BF16)
            lat_b[g] = narrow
            cache[0, g, own] = narrow
            lat_f[0, g] = jnp.where(pos < lengths[g], piece, 0.0)

    def latent_send(g):
        for d in range(1, seqs):
            z_copy(g, d).start()

    def latents_below(g):
        for d in range(1, seqs):

            @pl.when(seq >= d)
            def _():
                z_copy(g, d).wait_recv()

    def latents_above(g):
        for d in range(seqs - 1, 0, -1):

            @pl.when(seq < d)
            def _():
                z_copy(g, d).wait_recv()
                at = pl.ds(pl.multiple_of((seq - d + seqs) * rows, rows), rows)
                cache[0, g, at] = cache[1, g, at]

    def query_part(g0, ng, keys_t):
        span = slice(g0 * rows, (g0 + ng) * rows)
        query = jnp.dot(normed_s[span], wq_v[...], preferred_element_type=F32).astype(BF16)
        for h in range(heads_here):
            at = slice(h * HD, (h + 1) * HD)
            if keys_t is None:
                absorbed = dot_nt(query[:, at], wk_v[:, at])
            else:
                absorbed = jnp.dot(query[:, at], keys_t[at], preferred_element_type=F32)
            absorbed = (absorbed * scale).astype(BF16)
            for i in range(ng):
                absorbed_s[g0 + i, h * rows : (h + 1) * rows] = absorbed[i * rows : (i + 1) * rows]

    def take_input(g):
        waiter(part_in.at[:, g], h_recv.at[g]).wait_recv()
        half = rows // 2
        for r0 in range(0, rows, half):
            r = slice(r0, r0 + half)
            added = part_in[0, g, r].astype(F32)
            for source in range(1, heads):
                added = added + part_in[source, g, r].astype(F32)
            x = hid_v[g, r].astype(F32) + added
            x_s[g, r] = x
            normed_s[g * rows + r0 : g * rows + r0 + half] = rms_scale(x, gain[...]).astype(BF16)

    def project_later(g):
        take_input(g)
        latent_part(g, 1)
        latent_send(g)
        query_part(g, 1, wk_t)

    for d in range(1, seqs):

        @pl.when(seq + d < seqs)
        def _():
            at = pl.ds(pl.multiple_of((seq + d) * rows, rows), rows)
            for g in range(groups):
                cache[0, g, at] = jnp.zeros((rows, rank), BF16)

    loads[0].wait()
    for c in small:
        c.wait()

    @pl.when(first_sec)
    def _():
        half = rows // 2
        for g in range(groups):
            for r0 in range(0, rows, half):
                x = hid_v[g, r0 : r0 + half].astype(F32)
                normed_s[g * rows + r0 : g * rows + r0 + half] = rms_scale(x, gain[...]).astype(
                    BF16
                )
        loads[1].wait()
        latent_part(0, groups)

    pl.semaphore_wait(barrier, len(peers))

    key_pos = lax.broadcasted_iota(jnp.int32, (1, tok), 1)
    row_in = lax.broadcasted_iota(jnp.int32, (rows, 1), 0)
    mine = (row_in >= head * share) & (row_in < (head + 1) * share)

    def attend(g, last):
        keys = (g + 1) * tok
        per = heads_here
        while per > 2 and per * rows * keys > 512 * 768:
            per //= 2
        same = jnp.where(key_pos <= pos, 0.0, -1e30)
        same = jnp.concatenate([same] * per, axis=0)
        past = [jnp.where(key_pos < lengths[b], 0.0, -1e30) for b in range(g)]
        if g:
            latents_above(g - 1)
        latents_below(g)
        for h0 in range(0, heads_here, per):
            span = slice(h0 * rows, (h0 + per) * rows)
            scores = [dot_nt(absorbed_s[g, span], cache[0, b]) + past[b] for b in range(g)]
            scores.append(dot_nt(absorbed_s[g, span], cache[0, g]) + same)
            top = scores[0]
            for piece in scores[1:]:
                top = jnp.maximum(top, piece)
            top = jnp.max(top, axis=1, keepdims=True)
            total = None
            for b in range(g + 1):
                weights = jnp.exp(scores[b] - top)
                total = weights if total is None else total + weights
                weights_s[: per * rows, b * tok : (b + 1) * tok] = weights.astype(BF16)
            total = jnp.sum(total, axis=1, keepdims=True)
            accum = jnp.dot(
                weights_s[: per * rows, :keys],
                cache[0, : g + 1].reshape(keys, rank),
                preferred_element_type=F32,
            )
            context = (accum / total).astype(BF16)
            for i in range(0, per, 2):
                n = min(2, per - i)
                both = jnp.dot(
                    context[i * rows : (i + n) * rows],
                    wv_v[:, (h0 + i) * HD : (h0 + i + n) * HD],
                    preferred_element_type=F32,
                )
                for j in range(n):
                    at = slice((h0 + i + j) * HD, (h0 + i + j + 1) * HD)
                    attn_s[g, :, at] = both[
                        j * rows : (j + 1) * rows, j * HD : (j + 1) * HD
                    ].astype(BF16)

        for p in range(sections * sub):
            at = slice(p * cw, (p + 1) * cw)
            added = jnp.dot(attn_s[g], wo_v[:, at], preferred_element_type=F32)
            if last:
                state = x_s[g, :, at] + added
                x_s[g, :, at] = state
                added = jnp.where(mine, state, added)
            out_s[g, :, at] = added.astype(BF16)
            for dh in range(heads - 1, -1, -1):
                if not last:
                    h_copy(g, p, dh).start()
                elif (p, dh) in pairs:
                    f_copy(g, p, dh).start()

    @pl.when(first_sec)
    def _():
        for g in range(groups):
            for d in range(1, seqs):
                z_copy(g, d).start()
        loads[2].wait()
        loads[3].wait()
        query_part(0, groups, None)
        loads[4].wait()
        loads[5].wait()
        for g in range(groups):
            attend(g, False)

    @pl.when(jnp.logical_not(first_sec))
    def _():
        for c in loads[1:]:
            c.wait()
        wk_t[...] = wk_v[...].T
        for g in range(min(2, groups)):
            project_later(g)
        for g in range(groups):
            attend(g, True)
            if g + 2 < groups:
                project_later(g + 2)

    out_pos = seq * rows + head * share + lax.broadcasted_iota(jnp.int32, (share, 1), 0)
    my_rows = pl.ds(pl.multiple_of(head * share, share), share)
    my_cols = pl.ds(pl.multiple_of(sec * pw, pw), pw)
    for g in range(groups):

        @pl.when(last_sec)
        def _():
            waiter(fin_in.at[pl.ds(1, heads - 1), g], f_recv.at[g]).wait_recv()
            fin_v[g] = x_s[g, my_rows, my_cols]

        @pl.when(jnp.logical_not(last_sec))
        def _():
            waiter(fin_in.at[:, g], f_recv.at[g]).wait_recv()
            fin_v[g] = fin_in[0, g].astype(F32)

        value = fin_v[g]
        for dh in range(1, heads):
            value = value + fin_in[dh, g].astype(F32)
        fin_v[g] = jnp.where(out_pos < lengths[g], value, 0.0)

    for d in range(1, seqs):

        @pl.when(seq < d)
        def _():
            z_copy(groups - 1, d).wait_recv()

    waiter(cache.at[0, :, pl.ds(0, (seqs - 1) * rows)], z_send.at[0]).wait_send()

    @pl.when(jnp.logical_not(last_sec))
    def _():
        waiter(part_in, o_send.at[0]).wait_send()

    @pl.when(last_sec)
    def _():
        parts = sections * heads
        sent = width // parts * (parts - 1)
        waiter(out_s.at[:, :, pl.ds(0, sent)], o_send.at[0]).wait_send()


def flush(final_v, latents_v, final, latents, sem):
    copies = [
        pltpu.make_async_copy(final_v, final, sem.at[0]),
        pltpu.make_async_copy(latents_v, latents, sem.at[1]),
    ]
    for c in copies:
        c.start()
    for c in copies:
        c.wait()


def solution(mesh):
    seqs, sections, heads = mesh.shape["seq"], mesh.shape["section"], mesh.shape["head"]

    def shards(hidden, lengths, attn_gain, w_query, w_latent, latent_gain, w_key, w_value, w_out):
        groups, rows, width = hidden.shape
        rank = w_latent.shape[2]
        cols = w_query.shape[2]
        share, pw = rows // heads, width // sections
        hbm = pl.BlockSpec(memory_space=pltpu.HBM)
        vmem = pl.BlockSpec(memory_space=pltpu.VMEM)
        dma = pltpu.SemaphoreType.DMA
        final_v, latents_v = pl.pallas_call(
            functools.partial(kernel, (seqs, sections, heads)),
            out_shape=(
                pltpu.VMEM((groups, share, pw), F32),
                pltpu.VMEM((1, groups, rows, rank), F32),
            ),
            in_specs=[hbm] * 9,
            out_specs=(vmem, vmem),
            scratch_shapes=[
                pltpu.SMEM((groups,), jnp.int32),
                pltpu.VMEM((1, width), F32),
                pltpu.VMEM((1, rank), F32),
                pltpu.VMEM((groups, rows, width), BF16),
                pltpu.VMEM((width, cols), BF16),
                pltpu.VMEM((width, rank), BF16),
                pltpu.VMEM((rank, cols), BF16),
                pltpu.VMEM((cols, rank), BF16),
                pltpu.VMEM((rank, cols), BF16),
                pltpu.VMEM((cols, width), BF16),
                pltpu.VMEM((groups, rows, width), F32),
                pltpu.VMEM((groups * rows, width), BF16),
                pltpu.VMEM((groups, rows, rank), BF16),
                pltpu.VMEM((2, groups, rows * seqs, rank), BF16),
                pltpu.VMEM((groups, cols // HD * rows, rank), BF16),
                pltpu.VMEM((groups, rows, cols), BF16),
                pltpu.VMEM((groups, rows, width), BF16),
                pltpu.VMEM((heads, groups, rows, width), BF16),
                pltpu.VMEM((heads, groups, share, pw), BF16),
                pltpu.VMEM((cols // HD * rows, groups * rows * seqs), BF16),
                dma((9,)),
                dma((1,)),
                dma((groups, max(1, seqs - 1))),
                dma((1,)),
                dma((groups,)),
                dma((groups,)),
            ],
            compiler_params=pltpu.CompilerParams(
                collective_id=0, has_side_effects=True, vmem_limit_bytes=60 * 1024 * 1024
            ),
        )(lengths, hidden, attn_gain, latent_gain, w_query, w_latent, w_key, w_value, w_out)
        return pl.pallas_call(
            flush,
            out_shape=(
                jax.ShapeDtypeStruct(final_v.shape, F32),
                jax.ShapeDtypeStruct(latents_v.shape, F32),
            ),
            in_specs=[vmem] * 2,
            out_specs=(hbm, hbm),
            scratch_shapes=[dma((2,))],
            compiler_params=pltpu.CompilerParams(vmem_limit_bytes=1024 * 1024),
        )(final_v, latents_v)

    return jax.shard_map(
        shards,
        mesh=mesh,
        in_specs=(
            P("rep", "seq", None),
            P("rep"),
            P("section", None),
            P("section", None, "head"),
            P("section", None, None),
            P("section", None),
            P("section", None, "head"),
            P("section", None, "head"),
            P("section", "head", None),
        ),
        out_specs=(P("rep", ("seq", "head"), "section"), P("section", "rep", "seq", None)),
        check_vma=False,
    )
```

```python
import functools

import jax
import jax.numpy as jnp
from jax import lax
from jax.experimental import pallas as pl
from jax.experimental.pallas import tpu as pltpu
from jax.sharding import PartitionSpec as P

HD = 128
MESH = pl.DeviceIdType.MESH
F32 = jnp.float32
BF16 = jnp.bfloat16


def rms_scale(values, gain):
    mean_sq = jnp.mean(values * values, axis=-1, keepdims=True)
    return values * lax.rsqrt(mean_sq + 1e-06) * gain


def dot_nt(a, b):
    return lax.dot_general(a, b, (((1,), (1,)), ((), ())), preferred_element_type=F32)


def kernel(
    dims,
    lengths_h,
    hidden,
    gain_h,
    lgain_h,
    wq,
    wl,
    wk,
    wv,
    wo,
    fin_v,
    lat_f,
    lengths,
    gain,
    lgain,
    hid_v,
    wq_v,
    wl_v,
    wk_v,
    wk_t,
    wv_v,
    wo_v,
    x_s,
    normed_s,
    lat_b,
    cache,
    absorbed_s,
    attn_s,
    out_s,
    part_in,
    fin_in,
    weights_s,
    load_sem,
    z_send,
    z_recv,
    o_send,
    h_recv,
    f_recv,
):
    seqs, sections, heads = dims
    seq = lax.axis_index("seq")
    sec = lax.axis_index("section")
    head = lax.axis_index("head")
    groups, rows, width = hid_v.shape
    rank = wl_v.shape[1]
    cols = wq_v.shape[1]
    heads_here = cols // HD
    share = rows // heads
    pw = width // sections
    tok = rows * seqs
    scale = 1.0 / HD**0.5
    sub = 2
    cw = pw // sub
    first_sec = sec == 0
    last_sec = sec == sections - 1

    loads = [
        pltpu.make_async_copy(src, dst, load_sem.at[i])
        for i, (src, dst) in enumerate(
            [
                (hidden, hid_v),
                (wl.at[0], wl_v),
                (wq.at[0], wq_v),
                (wk.at[0], wk_v),
                (wv.at[0], wv_v),
                (wo.at[0], wo_v),
            ]
        )
    ]
    small = [
        pltpu.make_async_copy(src, dst, load_sem.at[6 + i])
        for i, (src, dst) in enumerate([(gain_h, gain), (lgain_h, lgain), (lengths_h, lengths)])
    ]
    loads[0].start()
    for c in small:
        c.start()
    for c in loads[1:]:
        c.start()

    barrier = pltpu.get_barrier_semaphore()
    peers = [{"seq": lax.rem(seq + d, seqs)} for d in range(1, seqs)]
    for ds in range(sections):
        for dh in range(heads):
            if ds or dh:
                peers.append(
                    {
                        "section": lax.rem(sec + ds, sections),
                        "head": lax.rem(head + dh, heads),
                    }
                )
    for peer in peers:
        pl.semaphore_signal(barrier, inc=1, device_id=peer, device_id_type=MESH)

    own = pl.ds(pl.multiple_of(seq * rows, rows), rows)
    pos = seq * rows + lax.broadcasted_iota(jnp.int32, (rows, 1), 0)

    def z_copy(g, d):
        return pltpu.make_async_remote_copy(
            src_ref=lat_b.at[g],
            dst_ref=cache.at[(seq + d) // seqs, g, own],
            send_sem=z_send.at[0],
            recv_sem=z_recv.at[g, d - 1],
            device_id={"seq": lax.rem(seq + d, seqs)},
            device_id_type=MESH,
        )

    def h_copy(g, p, dh):
        cols_p = pl.ds(p * cw, cw)
        return pltpu.make_async_remote_copy(
            src_ref=out_s.at[g, :, cols_p],
            dst_ref=part_in.at[head, g, :, cols_p],
            send_sem=o_send.at[0],
            recv_sem=h_recv.at[g],
            device_id={"section": lax.rem(sec + 1, sections), "head": lax.rem(head + dh, heads)},
            device_id_type=MESH,
        )

    def waiter(ref, sem):
        return pltpu.make_async_remote_copy(
            src_ref=ref,
            dst_ref=ref,
            send_sem=sem,
            recv_sem=sem,
            device_id={"section": lax.rem(sec + 1, sections)},
            device_id_type=MESH,
        )

    def f_copy(g, p, dh):
        to_head = lax.rem(head + dh, heads)
        return pltpu.make_async_remote_copy(
            src_ref=out_s.at[
                g, pl.ds(pl.multiple_of(to_head * share, share), share), pl.ds(p * cw, cw)
            ],
            dst_ref=fin_in.at[dh, g, :, pl.ds(p % sub * cw, cw)],
            send_sem=o_send.at[0],
            recv_sem=f_recv.at[g],
            device_id={"section": p // sub, "head": to_head},
            device_id_type=MESH,
        )

    pairs = [
        (p, dh)
        for p in range(sections * sub)
        for dh in range(heads)
        if p // sub < sections - 1 or dh
    ]

    def latent_part(g0, ng):
        span = slice(g0 * rows, (g0 + ng) * rows)
        raw = jnp.dot(normed_s[span], wl_v[...], preferred_element_type=F32)
        full = rms_scale(raw, lgain[...])
        for i in range(ng):
            g = g0 + i
            piece = full[i * rows : (i + 1) * rows]
            narrow = piece.astype(BF16)
            lat_b[g] = narrow
            cache[0, g, own] = narrow
            lat_f[0, g] = jnp.where(pos < lengths[g], piece, 0.0)

    def latent_send(g):
        for d in range(1, seqs):
            z_copy(g, d).start()

    def latents_below(g):
        for d in range(1, seqs):

            @pl.when(seq >= d)
            def _():
                z_copy(g, d).wait_recv()

    def latents_above(g):
        for d in range(seqs - 1, 0, -1):

            @pl.when(seq < d)
            def _():
                z_copy(g, d).wait_recv()
                at = pl.ds(pl.multiple_of((seq - d + seqs) * rows, rows), rows)
                cache[0, g, at] = cache[1, g, at]

    def query_part(g0, ng, keys_t):
        span = slice(g0 * rows, (g0 + ng) * rows)
        query = jnp.dot(normed_s[span], wq_v[...], preferred_element_type=F32).astype(BF16)
        for h in range(heads_here):
            at = slice(h * HD, (h + 1) * HD)
            if keys_t is None:
                absorbed = dot_nt(query[:, at], wk_v[:, at])
            else:
                absorbed = jnp.dot(query[:, at], keys_t[at], preferred_element_type=F32)
            absorbed = (absorbed * scale).astype(BF16)
            for i in range(ng):
                absorbed_s[g0 + i, h * rows : (h + 1) * rows] = absorbed[i * rows : (i + 1) * rows]

    def take_input(g):
        waiter(part_in.at[:, g], h_recv.at[g]).wait_recv()
        half = rows // 2
        for r0 in range(0, rows, half):
            r = slice(r0, r0 + half)
            added = part_in[0, g, r].astype(F32)
            for source in range(1, heads):
                added = added + part_in[source, g, r].astype(F32)
            x = hid_v[g, r].astype(F32) + added
            x_s[g, r] = x
            normed_s[g * rows + r0 : g * rows + r0 + half] = rms_scale(x, gain[...]).astype(BF16)

    def project_later(g):
        take_input(g)
        latent_part(g, 1)
        latent_send(g)
        query_part(g, 1, wk_t)

    for d in range(1, seqs):

        @pl.when(seq + d < seqs)
        def _():
            at = pl.ds(pl.multiple_of((seq + d) * rows, rows), rows)
            for g in range(groups):
                cache[0, g, at] = jnp.zeros((rows, rank), BF16)

    loads[0].wait()
    for c in small:
        c.wait()

    @pl.when(first_sec)
    def _():
        half = rows // 2
        for g in range(groups):
            for r0 in range(0, rows, half):
                x = hid_v[g, r0 : r0 + half].astype(F32)
                normed_s[g * rows + r0 : g * rows + r0 + half] = rms_scale(x, gain[...]).astype(
                    BF16
                )
        loads[1].wait()
        latent_part(0, groups)

    pl.semaphore_wait(barrier, len(peers))

    key_pos = lax.broadcasted_iota(jnp.int32, (1, tok), 1)
    row_in = lax.broadcasted_iota(jnp.int32, (rows, 1), 0)
    mine = (row_in >= head * share) & (row_in < (head + 1) * share)

    def attend(g, last):
        keys = (g + 1) * tok
        per = heads_here
        while per > 2 and per * rows * keys > 512 * 768:
            per //= 2
        same = jnp.where(key_pos <= pos, 0.0, -1e30)
        same = jnp.concatenate([same] * per, axis=0)
        past = [jnp.where(key_pos < lengths[b], 0.0, -1e30) for b in range(g)]
        if g:
            latents_above(g - 1)
        latents_below(g)
        for h0 in range(0, heads_here, per):
            span = slice(h0 * rows, (h0 + per) * rows)
            scores = [dot_nt(absorbed_s[g, span], cache[0, b]) + past[b] for b in range(g)]
            scores.append(dot_nt(absorbed_s[g, span], cache[0, g]) + same)
            top = scores[0]
            for piece in scores[1:]:
                top = jnp.maximum(top, piece)
            top = jnp.max(top, axis=1, keepdims=True)
            total = None
            for b in range(g + 1):
                weights = jnp.exp(scores[b] - top)
                total = weights if total is None else total + weights
                weights_s[: per * rows, b * tok : (b + 1) * tok] = weights.astype(BF16)
            total = jnp.sum(total, axis=1, keepdims=True)
            accum = jnp.dot(
                weights_s[: per * rows, :keys],
                cache[0, : g + 1].reshape(keys, rank),
                preferred_element_type=F32,
            )
            context = (accum / total).astype(BF16)
            for i in range(0, per, 2):
                n = min(2, per - i)
                both = jnp.dot(
                    context[i * rows : (i + n) * rows],
                    wv_v[:, (h0 + i) * HD : (h0 + i + n) * HD],
                    preferred_element_type=F32,
                )
                for j in range(n):
                    at = slice((h0 + i + j) * HD, (h0 + i + j + 1) * HD)
                    attn_s[g, :, at] = both[
                        j * rows : (j + 1) * rows, j * HD : (j + 1) * HD
                    ].astype(BF16)

        if not last:
            ahead = sub
        elif g + 1 < groups:
            ahead = sections * sub
        else:
            ahead = 1
        for p0 in range(0, sections * sub, ahead):
            at = slice(p0 * cw, (p0 + ahead) * cw)
            added = jnp.dot(attn_s[g], wo_v[:, at], preferred_element_type=F32)
            if last:
                state = x_s[g, :, at] + added
                x_s[g, :, at] = state
                added = jnp.where(mine, state, added)
            out_s[g, :, at] = added.astype(BF16)
            for p in range(p0, p0 + ahead):
                for dh in range(heads - 1, -1, -1):
                    if not last:
                        h_copy(g, p, dh).start()
                    elif (p, dh) in pairs:
                        f_copy(g, p, dh).start()

    @pl.when(first_sec)
    def _():
        for g in range(groups):
            for d in range(1, seqs):
                z_copy(g, d).start()
        loads[2].wait()
        loads[3].wait()
        query_part(0, groups, None)
        loads[4].wait()
        loads[5].wait()
        for g in range(groups):
            attend(g, False)

    @pl.when(jnp.logical_not(first_sec))
    def _():
        for c in loads[1:]:
            c.wait()
        wk_t[...] = wk_v[...].T
        for g in range(min(2, groups)):
            project_later(g)
        for g in range(groups):
            attend(g, True)
            if g + 2 < groups:
                project_later(g + 2)

    out_pos = seq * rows + head * share + lax.broadcasted_iota(jnp.int32, (share, 1), 0)
    my_rows = pl.ds(pl.multiple_of(head * share, share), share)
    my_cols = pl.ds(pl.multiple_of(sec * pw, pw), pw)
    for g in range(groups):

        @pl.when(last_sec)
        def _():
            waiter(fin_in.at[pl.ds(1, heads - 1), g], f_recv.at[g]).wait_recv()
            fin_v[g] = x_s[g, my_rows, my_cols]

        @pl.when(jnp.logical_not(last_sec))
        def _():
            waiter(fin_in.at[:, g], f_recv.at[g]).wait_recv()
            fin_v[g] = fin_in[0, g].astype(F32)

        value = fin_v[g]
        for dh in range(1, heads):
            value = value + fin_in[dh, g].astype(F32)
        fin_v[g] = jnp.where(out_pos < lengths[g], value, 0.0)

    for d in range(1, seqs):

        @pl.when(seq < d)
        def _():
            z_copy(groups - 1, d).wait_recv()

    waiter(cache.at[0, :, pl.ds(0, (seqs - 1) * rows)], z_send.at[0]).wait_send()

    @pl.when(jnp.logical_not(last_sec))
    def _():
        waiter(part_in, o_send.at[0]).wait_send()

    @pl.when(last_sec)
    def _():
        parts = sections * heads
        sent = width // parts * (parts - 1)
        waiter(out_s.at[:, :, pl.ds(0, sent)], o_send.at[0]).wait_send()


def flush(final_v, latents_v, final, latents, sem):
    copies = [
        pltpu.make_async_copy(final_v, final, sem.at[0]),
        pltpu.make_async_copy(latents_v, latents, sem.at[1]),
    ]
    for c in copies:
        c.start()
    for c in copies:
        c.wait()


def solution(mesh):
    seqs, sections, heads = mesh.shape["seq"], mesh.shape["section"], mesh.shape["head"]

    def shards(hidden, lengths, attn_gain, w_query, w_latent, latent_gain, w_key, w_value, w_out):
        groups, rows, width = hidden.shape
        rank = w_latent.shape[2]
        cols = w_query.shape[2]
        share, pw = rows // heads, width // sections
        hbm = pl.BlockSpec(memory_space=pltpu.HBM)
        vmem = pl.BlockSpec(memory_space=pltpu.VMEM)
        dma = pltpu.SemaphoreType.DMA
        final_v, latents_v = pl.pallas_call(
            functools.partial(kernel, (seqs, sections, heads)),
            out_shape=(
                pltpu.VMEM((groups, share, pw), F32),
                pltpu.VMEM((1, groups, rows, rank), F32),
            ),
            in_specs=[hbm] * 9,
            out_specs=(vmem, vmem),
            scratch_shapes=[
                pltpu.SMEM((groups,), jnp.int32),
                pltpu.VMEM((1, width), F32),
                pltpu.VMEM((1, rank), F32),
                pltpu.VMEM((groups, rows, width), BF16),
                pltpu.VMEM((width, cols), BF16),
                pltpu.VMEM((width, rank), BF16),
                pltpu.VMEM((rank, cols), BF16),
                pltpu.VMEM((cols, rank), BF16),
                pltpu.VMEM((rank, cols), BF16),
                pltpu.VMEM((cols, width), BF16),
                pltpu.VMEM((groups, rows, width), F32),
                pltpu.VMEM((groups * rows, width), BF16),
                pltpu.VMEM((groups, rows, rank), BF16),
                pltpu.VMEM((2, groups, rows * seqs, rank), BF16),
                pltpu.VMEM((groups, cols // HD * rows, rank), BF16),
                pltpu.VMEM((groups, rows, cols), BF16),
                pltpu.VMEM((groups, rows, width), BF16),
                pltpu.VMEM((heads, groups, rows, width), BF16),
                pltpu.VMEM((heads, groups, share, pw), BF16),
                pltpu.VMEM((cols // HD * rows, groups * rows * seqs), BF16),
                dma((9,)),
                dma((1,)),
                dma((groups, max(1, seqs - 1))),
                dma((1,)),
                dma((groups,)),
                dma((groups,)),
            ],
            compiler_params=pltpu.CompilerParams(
                collective_id=0, has_side_effects=True, vmem_limit_bytes=60 * 1024 * 1024
            ),
        )(lengths, hidden, attn_gain, latent_gain, w_query, w_latent, w_key, w_value, w_out)
        return pl.pallas_call(
            flush,
            out_shape=(
                jax.ShapeDtypeStruct(final_v.shape, F32),
                jax.ShapeDtypeStruct(latents_v.shape, F32),
            ),
            in_specs=[vmem] * 2,
            out_specs=(hbm, hbm),
            scratch_shapes=[dma((2,))],
            compiler_params=pltpu.CompilerParams(vmem_limit_bytes=1024 * 1024),
        )(final_v, latents_v)

    return jax.shard_map(
        shards,
        mesh=mesh,
        in_specs=(
            P("rep", "seq", None),
            P("rep"),
            P("section", None),
            P("section", None, "head"),
            P("section", None, None),
            P("section", None),
            P("section", None, "head"),
            P("section", None, "head"),
            P("section", "head", None),
        ),
        out_specs=(P("rep", ("seq", "head"), "section"), P("section", "rep", "seq", None)),
        check_vma=False,
    )
```

```python
import functools

import jax
import jax.numpy as jnp
from jax import lax
from jax.experimental import pallas as pl
from jax.experimental.pallas import tpu as pltpu
from jax.sharding import PartitionSpec as P

HD = 128
MESH = pl.DeviceIdType.MESH
F32 = jnp.float32
BF16 = jnp.bfloat16


def rms_scale(values, gain):
    mean_sq = jnp.mean(values * values, axis=-1, keepdims=True)
    return values * lax.rsqrt(mean_sq + 1e-06) * gain


def dot_nt(a, b):
    return lax.dot_general(a, b, (((1,), (1,)), ((), ())), preferred_element_type=F32)


def kernel(
    dims,
    lengths_h,
    hidden,
    gain_h,
    lgain_h,
    wq,
    wl,
    wk,
    wv,
    wo,
    fin_v,
    lat_f,
    lengths,
    gain,
    lgain,
    hid_v,
    wq_v,
    wl_v,
    wk_v,
    wk_t,
    wv_v,
    wo_v,
    x_s,
    normed_s,
    lat_b,
    cache,
    absorbed_s,
    attn_s,
    out_s,
    part_in,
    fin_in,
    weights_s,
    load_sem,
    z_send,
    z_recv,
    o_send,
    h_recv,
    f_recv,
):
    seqs, sections, heads = dims
    seq = lax.axis_index("seq")
    sec = lax.axis_index("section")
    head = lax.axis_index("head")
    groups, rows, width = hid_v.shape
    rank = wl_v.shape[1]
    cols = wq_v.shape[1]
    heads_here = cols // HD
    share = rows // heads
    pw = width // sections
    tok = rows * seqs
    scale = 1.0 / HD**0.5
    sub = 2
    cw = pw // sub
    first_sec = sec == 0
    last_sec = sec == sections - 1

    loads = [
        pltpu.make_async_copy(src, dst, load_sem.at[i])
        for i, (src, dst) in enumerate(
            [
                (hidden, hid_v),
                (wl.at[0], wl_v),
                (wq.at[0], wq_v),
                (wk.at[0], wk_v),
                (wv.at[0], wv_v),
                (wo.at[0], wo_v),
            ]
        )
    ]
    small = [
        pltpu.make_async_copy(src, dst, load_sem.at[6 + i])
        for i, (src, dst) in enumerate([(gain_h, gain), (lgain_h, lgain), (lengths_h, lengths)])
    ]
    loads[0].start()
    for c in small:
        c.start()
    for c in loads[1:]:
        c.start()

    barrier = pltpu.get_barrier_semaphore()
    peers = [{"seq": lax.rem(seq + d, seqs)} for d in range(1, seqs)]
    for ds in range(sections):
        for dh in range(heads):
            if ds or dh:
                peers.append(
                    {
                        "section": lax.rem(sec + ds, sections),
                        "head": lax.rem(head + dh, heads),
                    }
                )
    for peer in peers:
        pl.semaphore_signal(barrier, inc=1, device_id=peer, device_id_type=MESH)

    own = pl.ds(pl.multiple_of(seq * rows, rows), rows)
    pos = seq * rows + lax.broadcasted_iota(jnp.int32, (rows, 1), 0)

    def z_copy(g, d):
        return pltpu.make_async_remote_copy(
            src_ref=lat_b.at[g],
            dst_ref=cache.at[(seq + d) // seqs, g, own],
            send_sem=z_send.at[0],
            recv_sem=z_recv.at[g, d - 1],
            device_id={"seq": lax.rem(seq + d, seqs)},
            device_id_type=MESH,
        )

    def h_copy(g, p, dh):
        cols_p = pl.ds(p * cw, cw)
        return pltpu.make_async_remote_copy(
            src_ref=out_s.at[g, :, cols_p],
            dst_ref=part_in.at[head, g, :, cols_p],
            send_sem=o_send.at[0],
            recv_sem=h_recv.at[g],
            device_id={"section": lax.rem(sec + 1, sections), "head": lax.rem(head + dh, heads)},
            device_id_type=MESH,
        )

    def waiter(ref, sem):
        return pltpu.make_async_remote_copy(
            src_ref=ref,
            dst_ref=ref,
            send_sem=sem,
            recv_sem=sem,
            device_id={"section": lax.rem(sec + 1, sections)},
            device_id_type=MESH,
        )

    def f_copy(g, p, dh):
        to_head = lax.rem(head + dh, heads)
        return pltpu.make_async_remote_copy(
            src_ref=out_s.at[
                g, pl.ds(pl.multiple_of(to_head * share, share), share), pl.ds(p * cw, cw)
            ],
            dst_ref=fin_in.at[dh, g, :, pl.ds(p % sub * cw, cw)],
            send_sem=o_send.at[0],
            recv_sem=f_recv.at[g],
            device_id={"section": p // sub, "head": to_head},
            device_id_type=MESH,
        )

    pairs = [
        (p, dh)
        for p in range(sections * sub)
        for dh in range(heads)
        if p // sub < sections - 1 or dh
    ]

    def latent_part(g0, ng):
        span = slice(g0 * rows, (g0 + ng) * rows)
        raw = jnp.dot(normed_s[span], wl_v[...], preferred_element_type=F32)
        full = rms_scale(raw, lgain[...])
        for i in range(ng):
            g = g0 + i
            piece = full[i * rows : (i + 1) * rows]
            narrow = piece.astype(BF16)
            lat_b[g] = narrow
            cache[0, g, own] = narrow
            lat_f[0, g] = jnp.where(pos < lengths[g], piece, 0.0)

    def latent_send(g):
        for d in range(1, seqs):
            z_copy(g, d).start()

    def latents_below(g):
        for d in range(1, seqs):

            @pl.when(seq >= d)
            def _():
                z_copy(g, d).wait_recv()

    def latents_above(g):
        for d in range(seqs - 1, 0, -1):

            @pl.when(seq < d)
            def _():
                z_copy(g, d).wait_recv()
                at = pl.ds(pl.multiple_of((seq - d + seqs) * rows, rows), rows)
                cache[0, g, at] = cache[1, g, at]

    def query_part(g0, ng, keys_t):
        span = slice(g0 * rows, (g0 + ng) * rows)
        query = jnp.dot(normed_s[span], wq_v[...], preferred_element_type=F32).astype(BF16)
        for h in range(heads_here):
            at = slice(h * HD, (h + 1) * HD)
            if keys_t is None:
                absorbed = dot_nt(query[:, at], wk_v[:, at])
            else:
                absorbed = jnp.dot(query[:, at], keys_t[at], preferred_element_type=F32)
            absorbed = (absorbed * scale).astype(BF16)
            for i in range(ng):
                absorbed_s[g0 + i, h * rows : (h + 1) * rows] = absorbed[i * rows : (i + 1) * rows]

    def take_input(g):
        waiter(part_in.at[:, g], h_recv.at[g]).wait_recv()
        half = rows // 2
        for r0 in range(0, rows, half):
            r = slice(r0, r0 + half)
            added = part_in[0, g, r].astype(F32)
            for source in range(1, heads):
                added = added + part_in[source, g, r].astype(F32)
            x = hid_v[g, r].astype(F32) + added
            x_s[g, r] = x
            normed_s[g * rows + r0 : g * rows + r0 + half] = rms_scale(x, gain[...]).astype(BF16)

    def project_later(g):
        take_input(g)
        latent_part(g, 1)
        latent_send(g)
        query_part(g, 1, wk_t)

    for d in range(1, seqs):

        @pl.when(seq + d < seqs)
        def _():
            at = pl.ds(pl.multiple_of((seq + d) * rows, rows), rows)
            for g in range(groups):
                cache[0, g, at] = jnp.zeros((rows, rank), BF16)

    loads[0].wait()
    for c in small:
        c.wait()

    @pl.when(first_sec)
    def _():
        half = rows // 2
        for g in range(groups):
            for r0 in range(0, rows, half):
                x = hid_v[g, r0 : r0 + half].astype(F32)
                normed_s[g * rows + r0 : g * rows + r0 + half] = rms_scale(x, gain[...]).astype(
                    BF16
                )
        loads[1].wait()
        latent_part(0, groups)

    pl.semaphore_wait(barrier, len(peers))

    key_pos = lax.broadcasted_iota(jnp.int32, (1, tok), 1)
    row_in = lax.broadcasted_iota(jnp.int32, (rows, 1), 0)
    mine = (row_in >= head * share) & (row_in < (head + 1) * share)

    def attend(g, last):
        keys = (g + 1) * tok
        per = heads_here
        while per > 2 and per * rows * keys > 512 * 768:
            per //= 2
        same = jnp.where(key_pos <= pos, 0.0, -1e30)
        same = jnp.concatenate([same] * per, axis=0)
        past = [jnp.where(key_pos < lengths[b], 0.0, -1e30) for b in range(g)]
        if g:
            latents_above(g - 1)
        latents_below(g)
        for h0 in range(0, heads_here, per):
            span = slice(h0 * rows, (h0 + per) * rows)
            scores = [dot_nt(absorbed_s[g, span], cache[0, b]) + past[b] for b in range(g)]
            scores.append(dot_nt(absorbed_s[g, span], cache[0, g]) + same)
            top = scores[0]
            for piece in scores[1:]:
                top = jnp.maximum(top, piece)
            top = jnp.max(top, axis=1, keepdims=True)
            total = None
            for b in range(g + 1):
                weights = jnp.exp(scores[b] - top)
                total = weights if total is None else total + weights
                weights_s[: per * rows, b * tok : (b + 1) * tok] = weights.astype(BF16)
            total = jnp.sum(total, axis=1, keepdims=True)
            accum = jnp.dot(
                weights_s[: per * rows, :keys],
                cache[0, : g + 1].reshape(keys, rank),
                preferred_element_type=F32,
            )
            context = (accum / total).astype(BF16)
            for i in range(0, per, 2):
                n = min(2, per - i)
                both = jnp.dot(
                    context[i * rows : (i + n) * rows],
                    wv_v[:, (h0 + i) * HD : (h0 + i + n) * HD],
                    preferred_element_type=F32,
                )
                for j in range(n):
                    at = slice((h0 + i + j) * HD, (h0 + i + j + 1) * HD)
                    attn_s[g, :, at] = both[
                        j * rows : (j + 1) * rows, j * HD : (j + 1) * HD
                    ].astype(BF16)

        if not last:
            ahead = sub if g else 1
        elif g + 1 < groups:
            ahead = sections * sub
        else:
            ahead = 1
        for p0 in range(0, sections * sub, ahead):
            at = slice(p0 * cw, (p0 + ahead) * cw)
            added = jnp.dot(attn_s[g], wo_v[:, at], preferred_element_type=F32)
            if last:
                state = x_s[g, :, at] + added
                x_s[g, :, at] = state
                added = jnp.where(mine, state, added)
            out_s[g, :, at] = added.astype(BF16)
            for p in range(p0, p0 + ahead):
                for dh in range(heads - 1, -1, -1):
                    if not last:
                        h_copy(g, p, dh).start()
                    elif (p, dh) in pairs:
                        f_copy(g, p, dh).start()

    @pl.when(first_sec)
    def _():
        for g in range(groups):
            for d in range(1, seqs):
                z_copy(g, d).start()
        loads[2].wait()
        loads[3].wait()
        query_part(0, groups, None)
        loads[4].wait()
        loads[5].wait()
        for g in range(groups):
            attend(g, False)

    @pl.when(jnp.logical_not(first_sec))
    def _():
        for c in loads[1:]:
            c.wait()
        wk_t[...] = wk_v[...].T
        for g in range(min(2, groups)):
            project_later(g)
        for g in range(groups):
            attend(g, True)
            if g + 2 < groups:
                project_later(g + 2)

    out_pos = seq * rows + head * share + lax.broadcasted_iota(jnp.int32, (share, 1), 0)
    my_rows = pl.ds(pl.multiple_of(head * share, share), share)
    my_cols = pl.ds(pl.multiple_of(sec * pw, pw), pw)
    for g in range(groups):

        @pl.when(last_sec)
        def _():
            waiter(fin_in.at[pl.ds(1, heads - 1), g], f_recv.at[g]).wait_recv()
            fin_v[g] = x_s[g, my_rows, my_cols]

        @pl.when(jnp.logical_not(last_sec))
        def _():
            waiter(fin_in.at[:, g], f_recv.at[g]).wait_recv()
            fin_v[g] = fin_in[0, g].astype(F32)

        value = fin_v[g]
        for dh in range(1, heads):
            value = value + fin_in[dh, g].astype(F32)
        fin_v[g] = jnp.where(out_pos < lengths[g], value, 0.0)

    for d in range(1, seqs):

        @pl.when(seq < d)
        def _():
            z_copy(groups - 1, d).wait_recv()

    waiter(cache.at[0, :, pl.ds(0, (seqs - 1) * rows)], z_send.at[0]).wait_send()

    @pl.when(jnp.logical_not(last_sec))
    def _():
        waiter(part_in, o_send.at[0]).wait_send()

    @pl.when(last_sec)
    def _():
        parts = sections * heads
        sent = width // parts * (parts - 1)
        waiter(out_s.at[:, :, pl.ds(0, sent)], o_send.at[0]).wait_send()


def flush(final_v, latents_v, final, latents, sem):
    copies = [
        pltpu.make_async_copy(final_v, final, sem.at[0]),
        pltpu.make_async_copy(latents_v, latents, sem.at[1]),
    ]
    for c in copies:
        c.start()
    for c in copies:
        c.wait()


def solution(mesh):
    seqs, sections, heads = mesh.shape["seq"], mesh.shape["section"], mesh.shape["head"]

    def shards(hidden, lengths, attn_gain, w_query, w_latent, latent_gain, w_key, w_value, w_out):
        groups, rows, width = hidden.shape
        rank = w_latent.shape[2]
        cols = w_query.shape[2]
        share, pw = rows // heads, width // sections
        hbm = pl.BlockSpec(memory_space=pltpu.HBM)
        vmem = pl.BlockSpec(memory_space=pltpu.VMEM)
        dma = pltpu.SemaphoreType.DMA
        final_v, latents_v = pl.pallas_call(
            functools.partial(kernel, (seqs, sections, heads)),
            out_shape=(
                pltpu.VMEM((groups, share, pw), F32),
                pltpu.VMEM((1, groups, rows, rank), F32),
            ),
            in_specs=[hbm] * 9,
            out_specs=(vmem, vmem),
            scratch_shapes=[
                pltpu.SMEM((groups,), jnp.int32),
                pltpu.VMEM((1, width), F32),
                pltpu.VMEM((1, rank), F32),
                pltpu.VMEM((groups, rows, width), BF16),
                pltpu.VMEM((width, cols), BF16),
                pltpu.VMEM((width, rank), BF16),
                pltpu.VMEM((rank, cols), BF16),
                pltpu.VMEM((cols, rank), BF16),
                pltpu.VMEM((rank, cols), BF16),
                pltpu.VMEM((cols, width), BF16),
                pltpu.VMEM((groups, rows, width), F32),
                pltpu.VMEM((groups * rows, width), BF16),
                pltpu.VMEM((groups, rows, rank), BF16),
                pltpu.VMEM((2, groups, rows * seqs, rank), BF16),
                pltpu.VMEM((groups, cols // HD * rows, rank), BF16),
                pltpu.VMEM((groups, rows, cols), BF16),
                pltpu.VMEM((groups, rows, width), BF16),
                pltpu.VMEM((heads, groups, rows, width), BF16),
                pltpu.VMEM((heads, groups, share, pw), BF16),
                pltpu.VMEM((cols // HD * rows, groups * rows * seqs), BF16),
                dma((9,)),
                dma((1,)),
                dma((groups, max(1, seqs - 1))),
                dma((1,)),
                dma((groups,)),
                dma((groups,)),
            ],
            compiler_params=pltpu.CompilerParams(
                collective_id=0, has_side_effects=True, vmem_limit_bytes=60 * 1024 * 1024
            ),
        )(lengths, hidden, attn_gain, latent_gain, w_query, w_latent, w_key, w_value, w_out)
        return pl.pallas_call(
            flush,
            out_shape=(
                jax.ShapeDtypeStruct(final_v.shape, F32),
                jax.ShapeDtypeStruct(latents_v.shape, F32),
            ),
            in_specs=[vmem] * 2,
            out_specs=(hbm, hbm),
            scratch_shapes=[dma((2,))],
            compiler_params=pltpu.CompilerParams(vmem_limit_bytes=1024 * 1024),
        )(final_v, latents_v)

    return jax.shard_map(
        shards,
        mesh=mesh,
        in_specs=(
            P("rep", "seq", None),
            P("rep"),
            P("section", None),
            P("section", None, "head"),
            P("section", None, None),
            P("section", None),
            P("section", None, "head"),
            P("section", None, "head"),
            P("section", "head", None),
        ),
        out_specs=(P("rep", ("seq", "head"), "section"), P("section", "rep", "seq", None)),
        check_vma=False,
    )
```
